32 devices in a mesh: pop: 8 (over y, x, core), row: 4 (over z).
Axes of the slice: x: 2, y: 2, z: 4, core: 2. Of those that a mesh axis runs over, the one named last changes fastest.
Arguments:
- tokens: bfloat16 [384, 16, 4096], P('pop'), may hold values from -6 to 6
- weight: bfloat16 [14336, 4096], P('row', 'pop'), may hold values from -0.09375 to 0.09375
- bank_in: bfloat16 [4096, 128], P('row'), may hold values from -0.09375 to 0.09375
- bank_out: bfloat16 [14336, 128], P('row'), may hold values from -6 to 6
- fitness: int32 [384], P('pop'), may hold values from 0 to 191
- past_seeds: int32 [384, 2, 8], P('pop'), may hold values from 0 to 127
- new_seeds: int32 [384, 2, 8], P('pop'), may hold values from 0 to 127
Outputs:
- hidden: bfloat16 [384, 16, 14336], P('pop', None, 'row')
- new_weight: bfloat16 [14336, 4096], P('row', 'pop')
The draws below stay inside these ranges and needn't reach their ends.
All inputs are finite; a program needn't handle non-finite values.
Results may differ from the reference program's by a relative error of at most 0.012.
Values may be sent and summed in bfloat16 or wider, within the bound.
No kernel may reach another device: no remote copies, remote signals or barrier semaphores. Data moves between devices by JAX's collectives and lax.ppermute only.
A program may use at most 128 MiB of HBM per device.

```python
import jax
import jax.numpy as jnp
from jax import lax

D = 4096
FF = 14336
MEM_DEV = 48
TOK = 16
RANK = 8
BANK = 128
MEMBERS = 384
N_POP = 8


def touch_ends(drawn, key, smallest, largest):
    place = [jax.random.randint(jax.random.fold_in(key, axis), (), 0, length) for axis, length in enumerate(drawn.shape)]
    longest = drawn.shape.index(max(drawn.shape))
    neighbour = place[:longest] + [(place[longest] + 1) % drawn.shape[longest]] + place[longest + 1:]
    return drawn.at[tuple(place)].set(smallest).at[tuple(neighbour)].set(largest)


def steps_of(rng, dims, shards, smallest, high):
    gain, own = 1.0, jax.random.fold_in(rng, 6)
    for axis_at, blocks in shards:
        steps = jnp.exp(jax.random.uniform(jax.random.fold_in(own, axis_at), (blocks,), jnp.float32, smallest / len(shards), high / len(shards)))
        gain = gain * jnp.repeat(steps, dims[axis_at] // blocks).reshape([-1 if axis == axis_at else 1 for axis in range(len(dims))])
    return gain


def scatter_about(rng, extent, spread, limit, pieces=(), held_as=jnp.bfloat16):
    entries = jax.random.normal(rng, extent, jnp.float32) * spread
    if len(pieces) > 0:
        entries = steps_of(rng, extent, pieces, -0.22, 0.18) * entries
    return jnp.clip(entries, min=-limit, max=limit).astype(held_as)


def setup_inputs(seed: int = 0) -> dict:
    key_list = jax.random.split(jax.random.key(seed), 8)
    return {
        "tokens": scatter_about(key_list[0], (MEMBERS, TOK, D), 1.0, 6.0, ((0, 8),)),
        "weight": scatter_about(key_list[1], (FF, D), D ** -0.5, 0.09375, ((0, 4), (1, 8))),
        "bank_in": scatter_about(key_list[2], (D, BANK), D ** -0.5, 0.09375, ((0, 4),)),
        "bank_out": scatter_about(key_list[3], (FF, BANK), 1.0, 6.0, ((0, 4),)),
        "fitness": touch_ends(jax.random.randint(key_list[4], (MEMBERS,), 0, MEMBERS // 2), jax.random.fold_in(key_list[4], 1), 0, (MEMBERS // 2) - 1).astype(jnp.int32),
        "past_seeds": touch_ends(jax.random.randint(key_list[5], (MEMBERS, 2, RANK), 0, BANK), jax.random.fold_in(key_list[5], 1), 0, BANK - 1).astype(jnp.int32),
        "new_seeds": touch_ends(jax.random.randint(key_list[6], (MEMBERS, 2, RANK), 0, BANK), jax.random.fold_in(key_list[6], 1), 0, BANK - 1).astype(jnp.int32),
    }


NOISE_SCALE = 0.1
STEP_SCALE = 0.03


def one_hots(seeds):
    levels = jnp.arange(BANK, dtype=jnp.int32)
    out_hits = (seeds[:, 0, :, None] == levels).astype(jnp.float32)
    in_hits = (seeds[:, 1, :, None] == levels).astype(jnp.float32)
    return out_hits, in_hits


def reference(tokens, weight, bank_in, bank_out, fitness, past_seeds, new_seeds):
    lower_count = jnp.sum((fitness[None, :] < fitness[:, None]).astype(jnp.float32), axis=1)
    equal_count = jnp.sum((fitness[None, :] == fitness[:, None]).astype(jnp.float32), axis=1)
    centered = (lower_count + 0.5 * (equal_count - 1.0)) / (MEMBERS - 1.0) - 0.5
    out_hits, in_hits = one_hots(past_seeds)
    coupling = STEP_SCALE * jnp.einsum("m,mki,mkj->ij", centered, out_hits, in_hits)
    left_part = jnp.dot(bank_out.astype(jnp.float32), coupling, precision=lax.Precision.HIGHEST)
    update = jnp.dot(left_part, bank_in.astype(jnp.float32).T, precision=lax.Precision.HIGHEST)
    new_weight = (weight.astype(jnp.float32) + update).astype(jnp.bfloat16)
    grouped_tokens = tokens.reshape(N_POP, MEM_DEV, TOK, D)
    grouped_seeds = new_seeds.reshape(N_POP, MEM_DEV, 2, RANK)

    def forward(packed):
        member_tokens, member_seeds = packed
        flat_tokens = member_tokens.reshape(MEM_DEV * TOK, D)
        base_part = lax.dot_general(flat_tokens, new_weight, (((1,), (1,)), ((), ())), preferred_element_type=jnp.float32)
        projected = jnp.dot(flat_tokens, bank_in, preferred_element_type=jnp.float32).reshape(MEM_DEV, TOK, BANK)
        hidden_hits, feature_hits = one_hots(member_seeds)
        mixing = jnp.einsum("mkb,mkc->mbc", feature_hits, hidden_hits)
        low_term = (NOISE_SCALE * jnp.einsum("mtb,mbc->mtc", projected, mixing)).astype(jnp.bfloat16)
        extra = lax.dot_general(low_term.reshape(MEM_DEV * TOK, BANK), bank_out, (((1,), (1,)), ((), ())), preferred_element_type=jnp.float32)
        return (base_part + extra).astype(jnp.bfloat16).reshape(MEM_DEV, TOK, FF)

    hidden = lax.map(forward, (grouped_tokens, grouped_seeds)).reshape(MEMBERS, TOK, FF)
    return hidden, new_weight
```

```python
import functools

import jax
import jax.numpy as jnp
from jax import lax
from jax.experimental import pallas as pl
from jax.experimental.pallas import tpu as pltpu
from jax.sharding import PartitionSpec as P

NOISE_SCALE = 0.1
STEP_SCALE = 0.03


def one_hots(seeds, width):
    levels = jnp.arange(width, dtype=jnp.int32)
    out_hits = (seeds[:, 0, :, None] == levels).astype(jnp.float32)
    in_hits = (seeds[:, 1, :, None] == levels).astype(jnp.float32)
    return (out_hits, in_hits)


def flip(block, axis, mask, size):
    return lax.ppermute(block, axis, [(i, i ^ mask) for i in range(size)])


def cut(rows, tile):
    tiles = rows // tile
    if tiles < 8 or rows % tile:
        return [(0, rows)]
    last = 2
    half = tiles // 2
    lengths = [half - last, tiles - half - last, last, last]
    pieces, at = [], 0
    for length in lengths:
        pieces.append((at * tile, length * tile))
        at += length
    return pieces


def product_kernel(count, first, at_ref, tokens_ref, low_ref, bank_ref, *refs):
    blocks, out_ref = refs[:count], refs[-1]
    bank = bank_ref[...]
    dims = (((1,), (1,)), ((), ()))
    total = lax.dot_general(low_ref[...], jnp.concatenate([bank, bank], axis=1), dims, preferred_element_type=jnp.float32)
    for j, block_ref in enumerate(blocks):
        depth = block_ref.shape[1]
        columns = pl.ds(pl.multiple_of(at_ref[j] * depth, depth), depth)
        total += lax.dot_general(tokens_ref[:, columns], block_ref[...], dims, preferred_element_type=jnp.float32)
    out_ref[...] = total.astype(out_ref.dtype)


def product(hidden, at, tokens, low, bank_out, blocks, start, length, tile, rows):
    lines, width = tokens.shape[0], bank_out.shape[1]
    base = start // tile
    specs = [
        pl.BlockSpec(tokens.shape, lambda i, at: (0, 0)),
        pl.BlockSpec(low.shape, lambda i, at: (0, 0)),
        pl.BlockSpec((tile, width), lambda i, at: (base + i, 0)),
    ]
    for block, first in blocks:
        specs.append(pl.BlockSpec((tile, block.shape[1]), functools.partial(lambda i, at, skip: (skip + i, 0), skip=first // tile)))
    operands = [at, tokens, low, bank_out] + [block for block, _ in blocks]
    aliases = {}
    if hidden is not None:
        aliases = {len(operands): 0}
        operands.append(hidden)
        specs.append(pl.BlockSpec(memory_space=pl.ANY))
    features = tokens.shape[1]
    return pl.pallas_call(
        functools.partial(product_kernel, len(blocks), start),
        grid_spec=pltpu.PrefetchScalarGridSpec(
            num_scalar_prefetch=1,
            grid=(length // tile,),
            in_specs=specs,
            out_specs=pl.BlockSpec((lines, tile), lambda i, at: (0, base + i)),
        ),
        out_shape=jax.ShapeDtypeStruct((lines, rows), jnp.bfloat16),
        input_output_aliases=aliases,
        compiler_params=pltpu.CompilerParams(vmem_limit_bytes=32 * 1024 * 1024),
        cost_estimate=pl.CostEstimate(
            flops=2 * lines * length * (features + 2 * width),
            bytes_accessed=2 * (lines * features + length * features + lines * length),
            transcendentals=0,
        ),
        name="product",
    )(*operands)


def shards(tokens, weight, bank_in, bank_out, fitness, past_seeds, new_seeds):
    members = fitness.shape[0]
    pops, lanes = lax.axis_size("pop"), lax.axis_size("row")
    me, lane = lax.axis_index("pop"), lax.axis_index("row")
    overall = members * pops
    width = bank_out.shape[1]
    features = tokens.shape[2]
    rows, depth = weight.shape
    flat_tokens = tokens.reshape(members * tokens.shape[1], features)
    tile = 256
    chunks = cut(rows, tile)

    masks = [1 << b for b in range(pops.bit_length() - 1)]
    own = []
    source = weight
    for start, length in chunks:
        piece = source if length == rows else source[start : start + length]
        if len(own) == 0 and len(chunks) > 1:
            source, piece = lax.optimization_barrier((source, piece))
        own.append(piece)
    gathered = []
    partner = flip(weight, "pop", masks[0], pops)
    for c, (start, length) in enumerate(chunks):
        far = masks[1:]
        far = far[c % len(far) :] + far[: c % len(far)]
        here = {0: own[c]}
        for mask in far:
            here.update({m | mask: flip(b, "pop", mask, pops) for m, b in list(here.items())})
        for m in list(here):
            if m:
                here[m | masks[0]] = flip(here[m], "pop", masks[0], pops)
        here.pop(0)
        gathered.append({0: (weight, start), masks[0]: (partner, start), **{m: (b, 0) for m, b in here.items()}})

    packed = jnp.concatenate([fitness[:, None], past_seeds.reshape(members, -1)], axis=1)
    everyone = lax.all_gather(packed, "pop", axis=0, tiled=True)
    every_fitness = everyone[:, 0]
    every_seeds = everyone[:, 1:].reshape((overall,) + past_seeds.shape[1:])
    lower_count = jnp.sum((every_fitness[None, :] < every_fitness[:, None]).astype(jnp.float32), axis=1)
    equal_count = jnp.sum((every_fitness[None, :] == every_fitness[:, None]).astype(jnp.float32), axis=1)
    centered = (lower_count + 0.5 * (equal_count - 1.0)) / (overall - 1.0) - 0.5
    out_hits, in_hits = one_hots(every_seeds, width)
    scaled = (STEP_SCALE * centered)[:, None, None] * out_hits
    coupling = lax.dot_general(
        scaled.reshape(-1, width),
        in_hits.reshape(-1, width),
        (((0,), (0,)), ((), ())),
        precision=lax.Precision.HIGHEST,
    )

    span = bank_in.shape[0]
    full_in = jnp.zeros((features, width), bank_in.dtype)
    for step in range(lanes):
        block = bank_in if step == 0 else lax.ppermute(bank_in, "row", [(i, (i - step) % lanes) for i in range(lanes)])
        full_in = lax.dynamic_update_slice_in_dim(full_in, block, ((lane + step) % lanes) * span, 0)

    projected = jnp.dot(flat_tokens, full_in, preferred_element_type=jnp.float32)
    shift = lax.dot_general(projected, coupling, (((1,), (1,)), ((), ())), precision=lax.Precision.HIGHEST)
    hidden_hits, feature_hits = one_hots(new_seeds, width)
    mixing = jnp.einsum("mkb,mkc->mbc", feature_hits, hidden_hits)
    low_term = NOISE_SCALE * jnp.einsum("mtb,mbc->mtc", projected.reshape(members, -1, width), mixing)
    low = jnp.concatenate([low_term.reshape(-1, width).astype(jnp.bfloat16), shift.astype(jnp.bfloat16)], axis=1)

    left_part = jnp.dot(bank_out.astype(jnp.float32), coupling, precision=lax.Precision.HIGHEST)
    columns = lax.dynamic_slice_in_dim(full_in, me * depth, depth, 0).astype(jnp.float32)
    update = jnp.dot(left_part, columns.T, precision=lax.Precision.HIGHEST)
    new_weight = (weight.astype(jnp.float32) + update).astype(jnp.bfloat16)

    hidden = None
    for (start, length), blocks in zip(chunks, gathered):
        order = sorted(blocks)
        at = jnp.stack([me ^ m for m in order]).astype(jnp.int32)
        hidden = product(hidden, at, flat_tokens, low, bank_out, [blocks[m] for m in order], start, length, tile, rows)
    return (hidden.reshape(members, tokens.shape[1], rows), new_weight)


def solution(mesh):
    placed = (
        P("pop", None, None),
        P("row", "pop"),
        P("row", None),
        P("row", None),
        P("pop"),
        P("pop", None, None),
        P("pop", None, None),
    )
    return jax.shard_map(
        shards,
        mesh=mesh,
        in_specs=placed,
        out_specs=(P("pop", None, "row"), P("row", "pop")),
        check_vma=False,
    )
```

```python
import functools

import jax
import jax.numpy as jnp
from jax import lax
from jax.experimental import pallas as pl
from jax.experimental.pallas import tpu as pltpu
from jax.sharding import PartitionSpec as P


NOISE_SCALE = 0.1
STEP_SCALE = 0.03


def one_hots(seeds, width):
    levels = jnp.arange(width, dtype=jnp.int32)
    out_hits = (seeds[:, 0, :, None] == levels).astype(jnp.float32)
    in_hits = (seeds[:, 1, :, None] == levels).astype(jnp.float32)
    return (out_hits, in_hits)


DIMS = (((1,), (1,)), ((), ()))
LAST = 2
VMEM_LIMIT = 16 * 1024 * 1024


def cut(rows, tile):
    tiles = rows // tile
    if rows % tile or tiles < 6 or tiles % 2:
        return None
    last = min(LAST, tiles // 2 - 1)
    lengths = [tiles // 2 - last] * 2 + [last] * 2
    pieces, start = [], 0
    for length in lengths:
        pieces.append((start * tile, length * tile))
        start += length
    return pieces


def product_kernel(counts, half, tile, offset, final, resident, at_ref, tokens_ref, *refs):
    whole, split, with_low, with_partial = counts
    refs = list(refs)
    out_ref = refs.pop()
    step = pl.program_id(0)
    here = pl.ds(pl.multiple_of(step * tile, tile), tile)
    place = 0

    def term(block_ref, place):
        depth = block_ref.shape[1]
        columns = pl.ds(pl.multiple_of(at_ref[place] * depth, 128), depth)
        return lax.dot_general(tokens_ref[:, columns], block_ref[...], DIMS, preferred_element_type=jnp.float32)

    def store(value):
        if final:
            out_ref[...] = value.astype(out_ref.dtype)
        else:
            out_ref[:, here] = value

    total = None
    if with_low:
        low_ref, bank_ref = refs.pop(0), refs.pop(0)
        bank = bank_ref[...]
        total = lax.dot_general(low_ref[...], jnp.concatenate([bank, bank], axis=1), DIMS, preferred_element_type=jnp.float32)
    if with_partial:
        part = refs.pop(0)[:, pl.ds(pl.multiple_of(offset + step * tile, tile), tile)]
        total = part if total is None else total + part
    for place in whole:
        value = term(refs.pop(0), place)
        total = value if total is None else total + value
    if not split:
        store(total)
        return
    groups = [(places, (refs.pop(0), refs.pop(0))) for places in split]

    def finish(pick):
        done = total
        for places, pair in groups:
            block = pair[pick]
            if resident:
                block = block.at[pl.ds(pl.multiple_of((step - pick * half) * tile, tile), tile)]
            value = term(block, places[pick])
            done = value if done is None else done + value
        store(done)

    pl.when(step < half)(lambda: finish(0))
    pl.when(step >= half)(lambda: finish(1))


def product(at, tokens, start, length, tile, rows, whole=(), split=(), low=None, bank_out=None, partial=None, offset=0, final=False, hidden=None, resident=False):
    lines = tokens.shape[0]
    base, half = start // tile, length // tile // 2
    specs, operands, depth_sum = [pl.BlockSpec(memory_space=pltpu.VMEM)], [tokens], 0

    def add(operand, spec):
        operands.append(operand)
        specs.append(spec)

    if low is not None:
        add(low, pl.BlockSpec(memory_space=pltpu.VMEM))
        add(bank_out, pl.BlockSpec((tile, bank_out.shape[1]), lambda i, at: (base + i, 0)))
    if partial is not None:
        add(partial, pl.BlockSpec(memory_space=pltpu.VMEM))
    for place, block, first in whole:
        depth = block.shape[1]
        depth_sum += depth
        add(block, pl.BlockSpec((tile, depth), functools.partial(lambda i, at, skip: (skip + i, 0), skip=first // tile)))
    for _, upper, lower in split:
        depth = upper.shape[1]
        depth_sum += depth
        if resident:
            add(upper, pl.BlockSpec(memory_space=pltpu.VMEM))
            add(lower, pl.BlockSpec(memory_space=pltpu.VMEM))
            continue
        add(upper, pl.BlockSpec((tile, depth), lambda i, at: (jnp.minimum(i, half - 1), 0)))
        add(lower, pl.BlockSpec((tile, depth), lambda i, at: (jnp.maximum(i - half, 0), 0)))
    aliases = {}
    if hidden is not None:
        aliases = {len(operands) + 1: 0}
        add(hidden, pl.BlockSpec(memory_space=pl.ANY))
    counts = ([p for p, _, _ in whole], [p for p, _, _ in split], low is not None, partial is not None)

    def kernel(at_ref, *refs):
        refs = list(refs)
        if hidden is not None:
            refs.pop(-2)
        product_kernel(counts, half, tile, offset, final, resident, at_ref, *refs)

    if final:
        out_shape = jax.ShapeDtypeStruct((lines, rows), jnp.bfloat16)
        out_spec = pl.BlockSpec((lines, tile), lambda i, at: (0, base + i))
    else:
        out_shape = jax.ShapeDtypeStruct((lines, length), jnp.float32)
        out_spec = pl.BlockSpec(memory_space=pltpu.VMEM)
    return pl.pallas_call(
        kernel,
        grid_spec=pltpu.PrefetchScalarGridSpec(num_scalar_prefetch=1, grid=(length // tile,), in_specs=specs, out_specs=out_spec),
        out_shape=out_shape,
        input_output_aliases=aliases,
        compiler_params=pltpu.CompilerParams(vmem_limit_bytes=VMEM_LIMIT),
        cost_estimate=pl.CostEstimate(
            flops=2 * lines * length * depth_sum,
            bytes_accessed=2 * (lines * depth_sum + length * depth_sum + lines * length),
            transcendentals=0,
        ),
    )(at, *operands)


def take_kernel(pieces, source_ref, *refs):
    outs, sems = refs[: len(pieces)], refs[len(pieces)]
    copies = [pltpu.make_async_copy(source_ref.at[pl.ds(start, length)], out, sems.at[j]) for j, ((start, length), out) in enumerate(zip(pieces, outs))]
    for copy in copies:
        copy.start()
    for copy in copies:
        copy.wait()


def take(source, pieces):
    depth = source.shape[1]
    size = sum(length for _, length in pieces) * depth * 2
    return pl.pallas_call(
        functools.partial(take_kernel, pieces),
        in_specs=[pl.BlockSpec(memory_space=pl.ANY)],
        out_specs=[pl.BlockSpec(memory_space=pltpu.VMEM)] * len(pieces),
        out_shape=[jax.ShapeDtypeStruct((length, depth), source.dtype) for _, length in pieces],
        scratch_shapes=[pltpu.SemaphoreType.DMA((len(pieces),))],
        compiler_params=pltpu.CompilerParams(vmem_limit_bytes=VMEM_LIMIT),
        cost_estimate=pl.CostEstimate(flops=size, bytes_accessed=2 * size, transcendentals=0),
    )(source)


def update_kernel(weight_ref, bank_ref, right_ref, out_ref):
    bank = bank_ref[...]
    update = jnp.dot(jnp.concatenate([bank, bank], axis=1), right_ref[...], preferred_element_type=jnp.float32)
    out_ref[...] = (weight_ref[...].astype(jnp.float32) + update).astype(out_ref.dtype)


def updated(weight, bank_out, right_part):
    rows, depth = weight.shape
    width = bank_out.shape[1]
    tile = rows // 4 if rows % 64 == 0 else rows
    return pl.pallas_call(
        update_kernel,
        grid=(rows // tile,),
        in_specs=[
            pl.BlockSpec((tile, depth), lambda i: (i, 0)),
            pl.BlockSpec((tile, width), lambda i: (i, 0)),
            pl.BlockSpec(right_part.shape, lambda i: (0, 0)),
        ],
        out_specs=pl.BlockSpec((tile, depth), lambda i: (i, 0)),
        out_shape=jax.ShapeDtypeStruct(weight.shape, weight.dtype),
        compiler_params=pltpu.CompilerParams(vmem_limit_bytes=12 * 1024 * 1024),
        cost_estimate=pl.CostEstimate(flops=4 * rows * depth * width, bytes_accessed=4 * rows * depth, transcendentals=0),
        name="update",
    )(weight, bank_out, right_part)


def project_kernel(steps, pick_ref, tokens_ref, *refs):
    blocks, out_ref, columns_ref = refs[:steps], refs[steps], refs[steps + 1]
    total = None
    for j, block_ref in enumerate(blocks):
        span = block_ref.shape[0]
        place = pl.ds(pl.multiple_of(pick_ref[j] * span, 128), span)
        term = jnp.dot(tokens_ref[:, place], block_ref[...], preferred_element_type=jnp.float32)
        total = term if total is None else total + term
    out_ref[...] = total
    depth = columns_ref.shape[0]
    for j, block_ref in enumerate(blocks):

        @pl.when((pl.program_id(0) == 0) & (pick_ref[steps] == pick_ref[j]))
        def _(block_ref=block_ref):
            columns_ref[...] = block_ref[pl.ds(pl.multiple_of(pick_ref[steps + 1], 16), depth), :]


def projections(pick, tokens, blocks, depth):
    lines, features = tokens.shape
    width = blocks[0].shape[1]
    tile = 256 if lines % 256 == 0 else lines
    return pl.pallas_call(
        functools.partial(project_kernel, len(blocks)),
        grid_spec=pltpu.PrefetchScalarGridSpec(
            num_scalar_prefetch=1,
            grid=(lines // tile,),
            in_specs=[pl.BlockSpec((tile, features), lambda i, pick: (i, 0))]
            + [pl.BlockSpec(b.shape, lambda i, pick: (0, 0)) for b in blocks],
            out_specs=[pl.BlockSpec((tile, width), lambda i, pick: (i, 0)), pl.BlockSpec((depth, width), lambda i, pick: (0, 0))],
        ),
        out_shape=[jax.ShapeDtypeStruct((lines, width), jnp.float32), jax.ShapeDtypeStruct((depth, width), blocks[0].dtype)],
        compiler_params=pltpu.CompilerParams(vmem_limit_bytes=16 * 1024 * 1024),
        cost_estimate=pl.CostEstimate(flops=2 * lines * features * width, bytes_accessed=2 * lines * features, transcendentals=0),
        name="project",
    )(pick, tokens, *blocks)


def lowrank_kernel(ranks, projected_ref, coupling_ref, seeds_ref, columns_ref, low_ref, right_ref):
    projected, coupling = projected_ref[...], coupling_ref[...]
    members = seeds_ref.shape[0]
    lines, width = projected.shape
    grouped = projected.reshape(members, lines // members, width)
    levels = lax.broadcasted_iota(jnp.int32, (members, 1, width), 2)
    mixed = None
    for k in range(ranks):
        feature_hit = (seeds_ref[:, 1:2, k : k + 1] == levels).astype(jnp.float32)
        hidden_hit = (seeds_ref[:, 0:1, k : k + 1] == levels).astype(jnp.float32)
        term = jnp.sum(grouped * feature_hit, axis=2, keepdims=True) * hidden_hit
        mixed = term if mixed is None else mixed + term
    low_ref[:, :width] = (NOISE_SCALE * mixed).reshape(lines, width).astype(low_ref.dtype)
    shift = lax.dot_general(projected, coupling, DIMS, precision=lax.Precision.HIGHEST, preferred_element_type=jnp.float32)
    low_ref[:, width:] = shift.astype(low_ref.dtype)
    right = lax.dot_general(coupling, columns_ref[...].astype(jnp.float32), DIMS, precision=lax.Precision.HIGHEST, preferred_element_type=jnp.float32)
    upper = right.astype(right_ref.dtype)
    right_ref[:width, :] = upper
    right_ref[width:, :] = (right - upper.astype(jnp.float32)).astype(right_ref.dtype)


def lowrank(projected, coupling, seeds, columns):
    lines, width = projected.shape
    depth = columns.shape[0]
    return pl.pallas_call(
        functools.partial(lowrank_kernel, seeds.shape[2]),
        out_shape=[jax.ShapeDtypeStruct((lines, 2 * width), jnp.bfloat16), jax.ShapeDtypeStruct((2 * width, depth), jnp.bfloat16)],
        compiler_params=pltpu.CompilerParams(vmem_limit_bytes=16 * 1024 * 1024),
        cost_estimate=pl.CostEstimate(flops=20 * lines * width * width, bytes_accessed=8 * lines * width, transcendentals=0),
        name="lowrank",
    )(projected, coupling, seeds, columns)


def shards(tokens, weight, bank_in, bank_out, fitness, past_seeds, new_seeds):
    members = fitness.shape[0]
    pops, lanes = lax.axis_size("pop"), lax.axis_size("row")
    me, lane = lax.axis_index("pop"), lax.axis_index("row")
    overall = members * pops
    width = bank_out.shape[1]
    features = tokens.shape[2]
    rows, depth = weight.shape
    flat_tokens = tokens.reshape(members * tokens.shape[1], features)
    tile = 256
    chunks = cut(rows, tile)
    planned = pops == 8 and chunks is not None

    def flip(block, mask):
        return lax.ppermute(block, "pop", [(i, i ^ mask) for i in range(pops)])

    at = (me ^ jnp.arange(pops, dtype=jnp.int32)).astype(jnp.int32)
    packed = jnp.concatenate([fitness[:, None], past_seeds.reshape(members, -1)], axis=1)

    held = {}
    if planned:
        core, one, two = 1, 2, 4
        own = take(weight, chunks[:1]) + take(weight, chunks[1:])
        for c, piece in enumerate(own):
            held[c, one] = flip(piece, one)
            held[c, two] = flip(piece, two)
        partner = flip(weight, core)
        for c in range(len(chunks)):
            held[c, one | two] = flip(held[c, two], one) if c % 2 else flip(held[c, one], two)
            for mask in (one, two, one | two):
                held[c, mask | core] = flip(held[c, mask], core)
        both = jnp.concatenate([packed, flip(packed, core)], axis=0)
        side = lax.ppermute(both, "pop", [(i, i ^ (two if i & core else one)) for i in range(pops)])
        across = lax.ppermute(both, "pop", [(i, i ^ (one | two)) for i in range(0, pops, 2)])
        mine = jnp.concatenate([side, across], axis=0)
        theirs = flip(mine, core)
        rest = both.shape[0]
        everyone = jnp.concatenate([both, side, theirs[:rest], across + theirs[rest:]], axis=0)
    else:
        everyone = lax.all_gather(packed, "pop", axis=0, tiled=True)

    every_fitness = everyone[:, 0]
    every_seeds = everyone[:, 1:].reshape((overall,) + past_seeds.shape[1:])
    lower_count = jnp.sum((every_fitness[None, :] < every_fitness[:, None]).astype(jnp.float32), axis=1)
    equal_count = jnp.sum((every_fitness[None, :] == every_fitness[:, None]).astype(jnp.float32), axis=1)
    centered = (lower_count + 0.5 * (equal_count - 1.0)) / (overall - 1.0) - 0.5
    out_hits, in_hits = one_hots(every_seeds, width)
    scaled = (STEP_SCALE * centered)[:, None, None] * out_hits
    coupling = lax.dot_general(
        scaled.reshape(-1, width),
        in_hits.reshape(-1, width),
        (((0,), (0,)), ((), ())),
        precision=lax.Precision.HIGHEST,
    )

    span = bank_in.shape[0]
    banks = [bank_in]
    for step in range(1, lanes):
        banks.append(lax.ppermute(bank_in, "row", [(i, (i - step) % lanes) for i in range(lanes)]))
    if span % depth == 0:
        ring = (lane + jnp.arange(lanes, dtype=jnp.int32)) % lanes
        pick = jnp.concatenate([ring, jnp.stack([me * depth // span, me * depth % span])]).astype(jnp.int32)
        projected, columns = projections(pick, flat_tokens, banks, depth)
    else:
        full_in = jnp.zeros((features, width), bank_in.dtype)
        for step, block in enumerate(banks):
            full_in = lax.dynamic_update_slice_in_dim(full_in, block, ((lane + step) % lanes) * span, 0)
        projected = jnp.dot(flat_tokens, full_in, preferred_element_type=jnp.float32)
        columns = lax.dynamic_slice_in_dim(full_in, me * depth, depth, 0)
    low, right_part = lowrank(projected, coupling, new_seeds, columns)
    new_weight = updated(weight, bank_out, right_part)

    if planned:
        hidden = None

        def pair(c, upper, lower):
            return [((u, l), held[c, u], held[c + 1, l]) for u, l in zip(upper, lower)]

        def wide(c):
            start = chunks[c][0]
            return dict(start=start, length=2 * chunks[c][1], tile=tile, rows=rows), [(0, weight, start), (core, partner, start)]

        sizes, own = wide(0)
        partial = product(at, flat_tokens, **sizes, whole=own, split=pair(0, (2, 3, 4, 5), (2, 3, 4, 5)), low=low, bank_out=bank_out)
        for c in (0, 1):
            start, length = chunks[c]
            far = [(m, held[c, m], 0) for m in (6, 7)]
            hidden = product(at, flat_tokens, start, length, tile, rows, whole=far, partial=partial, offset=start, final=True, hidden=hidden)
        sizes, own = wide(2)
        partial = product(at, flat_tokens, **sizes, whole=own, split=pair(2, (2, 3), (4, 5)), low=low, bank_out=bank_out)
        partial = product(at, flat_tokens, **sizes, split=pair(2, (4, 5), (2, 3)), partial=partial)
        hidden = product(at, flat_tokens, **sizes, split=pair(2, (6, 7), (6, 7)), partial=partial, final=True, hidden=hidden, resident=True)
    else:
        blocks = {0: weight}
        for bit in range((pops - 1).bit_length()):
            if pops & (pops - 1) == 0:
                blocks.update({m | 1 << bit: flip(b, 1 << bit) for m, b in list(blocks.items())})
        if len(blocks) == pops:
            full = jnp.zeros((rows, features), weight.dtype)
            for m, b in blocks.items():
                full = lax.dynamic_update_slice_in_dim(full, b, (me ^ m) * depth, 1)
        else:
            full = lax.all_gather(weight, "pop", axis=1, tiled=True)
        hidden = lax.dot_general(flat_tokens, full, DIMS, preferred_element_type=jnp.float32)
        hidden += lax.dot_general(low, jnp.concatenate([bank_out, bank_out], axis=1), DIMS, preferred_element_type=jnp.float32)
        hidden = hidden.astype(jnp.bfloat16)
    return (hidden.reshape(members, tokens.shape[1], rows), new_weight)


def solution(mesh):
    placed = (
        P("pop", None, None),
        P("row", "pop"),
        P("row", None),
        P("row", None),
        P("pop"),
        P("pop", None, None),
        P("pop", None, None),
    )
    return jax.shard_map(
        shards,
        mesh=mesh,
        in_specs=placed,
        out_specs=(P("pop", None, "row"), P("row", "pop")),
        check_vma=False,
    )
```

```python
import functools

import jax
import jax.numpy as jnp
from jax import lax
from jax.experimental import pallas as pl
from jax.experimental.pallas import tpu as pltpu
from jax.sharding import PartitionSpec as P


NOISE_SCALE = 0.1
STEP_SCALE = 0.03


def one_hots(seeds, width):
    levels = jnp.arange(width, dtype=jnp.int32)
    out_hits = (seeds[:, 0, :, None] == levels).astype(jnp.float32)
    in_hits = (seeds[:, 1, :, None] == levels).astype(jnp.float32)
    return (out_hits, in_hits)


DIMS = (((1,), (1,)), ((), ()))
TILE = 256
CORE, ONE, TWO = 1, 2, 4
VMEM_LIMIT = 10 * 1024 * 1024


def cut(rows, tile):
    tiles = rows // tile
    if rows % tile or tiles < 8:
        return None
    second = (tiles - 4) * 3 // 10
    lengths = [tiles - 4 - second, second, 2, 2]
    pieces, start = [], 0
    for length in lengths:
        pieces.append((start * tile, length * tile))
        start += length
    return pieces


def source_of(place, me):
    swap = (me ^ place) & CORE
    there = place & CORE
    for axis in (ONE, TWO):
        if place & axis:
            there = there ^ (axis + swap * ((axis ^ ONE ^ TWO) - axis))
    return me ^ there


def product_kernel(places, tile, with_low, with_partial, final, resident, tokens_ref, *refs):
    refs = list(refs)
    out_ref = refs.pop()
    me = lax.axis_index("pop")
    here = pl.ds(pl.multiple_of(pl.program_id(0) * tile, tile), tile)
    total = None
    if with_low:
        low_ref, bank_ref = refs.pop(0), refs.pop(0)
        bank = bank_ref[...]
        total = lax.dot_general(low_ref[...], jnp.concatenate([bank, bank], axis=1), DIMS, preferred_element_type=jnp.float32)
    if with_partial:
        total = refs.pop(0)[:, here]
    for place, block_ref in zip(places, refs):
        depth = block_ref.shape[1]
        columns = pl.ds(pl.multiple_of(source_of(place, me) * depth, 128), depth)
        block = block_ref[here, :] if resident else block_ref[...]
        term = lax.dot_general(tokens_ref[:, columns], block, DIMS, preferred_element_type=jnp.float32)
        total = term if total is None else total + term
    if final:
        out_ref[...] = total.astype(out_ref.dtype)
    else:
        out_ref[:, here] = total


def product(tokens, start, length, tile, rows, blocks, low=None, bank_out=None, partial=None, hidden=None, resident=False):
    lines = tokens.shape[0]
    base, final = start // tile, partial is not None
    specs, operands, depth_sum = [pl.BlockSpec(memory_space=pltpu.VMEM)], [tokens], 0

    def add(operand, spec):
        operands.append(operand)
        specs.append(spec)

    if low is not None:
        add(low, pl.BlockSpec(memory_space=pltpu.VMEM))
        add(bank_out, pl.BlockSpec((tile, bank_out.shape[1]), lambda i: (base + i, 0)))
    if final:
        add(partial, pl.BlockSpec(memory_space=pltpu.VMEM))
    for _, block, first in blocks:
        depth = block.shape[1]
        depth_sum += depth
        if resident:
            add(block, pl.BlockSpec(memory_space=pltpu.VMEM))
        else:
            add(block, pl.BlockSpec((tile, depth), functools.partial(lambda i, skip: (skip + i, 0), skip=first // tile)))
    aliases = {}
    if hidden is not None:
        aliases = {len(operands): 0}
        add(hidden, pl.BlockSpec(memory_space=pl.ANY))
    places = [place for place, _, _ in blocks]

    def kernel(*refs):
        refs = list(refs)
        if hidden is not None:
            refs.pop(-2)
        product_kernel(places, tile, low is not None, final, final, resident, *refs)

    if final:
        out_shape = jax.ShapeDtypeStruct((lines, rows), jnp.bfloat16)
        out_spec = pl.BlockSpec((lines, tile), lambda i: (0, base + i))
    else:
        out_shape = jax.ShapeDtypeStruct((lines, length), jnp.float32)
        out_spec = pl.BlockSpec(memory_space=pltpu.VMEM)
    return pl.pallas_call(
        kernel,
        grid=(length // tile,),
        in_specs=specs,
        out_specs=out_spec,
        out_shape=out_shape,
        input_output_aliases=aliases,
        compiler_params=pltpu.CompilerParams(vmem_limit_bytes=VMEM_LIMIT),
        cost_estimate=pl.CostEstimate(
            flops=2 * lines * length * depth_sum,
            bytes_accessed=2 * (lines * depth_sum + length * depth_sum + lines * length),
            transcendentals=0,
        ),
    )(*operands)


def take_kernel(pieces, source_ref, *refs):
    outs, sems = refs[: len(pieces)], refs[len(pieces)]
    copies = []
    for (start, length), out in zip(pieces, outs):
        for at in range(0, length, TILE):
            copies.append(pltpu.make_async_copy(source_ref.at[pl.ds(start + at, TILE)], out.at[pl.ds(at, TILE)], sems.at[len(copies)]))
    for copy in copies:
        copy.start()
    for copy in copies:
        copy.wait()


def take(source, pieces):
    depth = source.shape[1]
    size = sum(length for _, length in pieces) * depth * 2
    return pl.pallas_call(
        functools.partial(take_kernel, pieces),
        in_specs=[pl.BlockSpec(memory_space=pl.ANY)],
        out_specs=[pl.BlockSpec(memory_space=pltpu.VMEM)] * len(pieces),
        out_shape=[jax.ShapeDtypeStruct((length, depth), source.dtype) for _, length in pieces],
        scratch_shapes=[pltpu.SemaphoreType.DMA((sum(length for _, length in pieces) // TILE,))],
        compiler_params=pltpu.CompilerParams(vmem_limit_bytes=VMEM_LIMIT),
        cost_estimate=pl.CostEstimate(flops=size, bytes_accessed=2 * size, transcendentals=0),
    )(source)


def update_kernel(weight_ref, bank_ref, right_ref, out_ref):
    bank = bank_ref[...]
    update = jnp.dot(jnp.concatenate([bank, bank], axis=1), right_ref[...], preferred_element_type=jnp.float32)
    out_ref[...] = (weight_ref[...].astype(jnp.float32) + update).astype(out_ref.dtype)


def updated(weight, bank_out, right_part):
    rows, depth = weight.shape
    width = bank_out.shape[1]
    tile = rows // 4 if rows % 64 == 0 else rows
    return pl.pallas_call(
        update_kernel,
        grid=(rows // tile,),
        in_specs=[
            pl.BlockSpec((tile, depth), lambda i: (i, 0)),
            pl.BlockSpec((tile, width), lambda i: (i, 0)),
            pl.BlockSpec(right_part.shape, lambda i: (0, 0)),
        ],
        out_specs=pl.BlockSpec((tile, depth), lambda i: (i, 0)),
        out_shape=jax.ShapeDtypeStruct(weight.shape, weight.dtype),
        compiler_params=pltpu.CompilerParams(vmem_limit_bytes=VMEM_LIMIT),
        cost_estimate=pl.CostEstimate(flops=4 * rows * depth * width, bytes_accessed=4 * rows * depth, transcendentals=0),
        name="update",
    )(weight, bank_out, right_part)


def project_kernel(steps, pick_ref, tokens_ref, *refs):
    blocks, out_ref, columns_ref = refs[:steps], refs[steps], refs[steps + 1]
    total = None
    for j, block_ref in enumerate(blocks):
        span = block_ref.shape[0]
        place = pl.ds(pl.multiple_of(pick_ref[j] * span, 128), span)
        term = jnp.dot(tokens_ref[:, place], block_ref[...], preferred_element_type=jnp.float32)
        total = term if total is None else total + term
    out_ref[...] = total
    depth = columns_ref.shape[0]
    for j, block_ref in enumerate(blocks):

        @pl.when((pl.program_id(0) == 0) & (pick_ref[steps] == pick_ref[j]))
        def _(block_ref=block_ref):
            columns_ref[...] = block_ref[pl.ds(pl.multiple_of(pick_ref[steps + 1], 16), depth), :]


def projections(pick, tokens, blocks, depth):
    lines, features = tokens.shape
    width = blocks[0].shape[1]
    tile = 256 if lines % 256 == 0 else lines
    return pl.pallas_call(
        functools.partial(project_kernel, len(blocks)),
        grid_spec=pltpu.PrefetchScalarGridSpec(
            num_scalar_prefetch=1,
            grid=(lines // tile,),
            in_specs=[pl.BlockSpec((tile, features), lambda i, pick: (i, 0))]
            + [pl.BlockSpec(b.shape, lambda i, pick: (0, 0)) for b in blocks],
            out_specs=[pl.BlockSpec((tile, width), lambda i, pick: (i, 0)), pl.BlockSpec((depth, width), lambda i, pick: (0, 0))],
        ),
        out_shape=[jax.ShapeDtypeStruct((lines, width), jnp.float32), jax.ShapeDtypeStruct((depth, width), blocks[0].dtype)],
        compiler_params=pltpu.CompilerParams(vmem_limit_bytes=VMEM_LIMIT),
        cost_estimate=pl.CostEstimate(flops=2 * lines * features * width, bytes_accessed=2 * lines * features, transcendentals=0),
        name="project",
    )(pick, tokens, *blocks)


def lowrank_kernel(ranks, projected_ref, coupling_ref, seeds_ref, columns_ref, low_ref, right_ref):
    projected, coupling = projected_ref[...], coupling_ref[...]
    members = seeds_ref.shape[0]
    lines, width = projected.shape
    grouped = projected.reshape(members, lines // members, width)
    levels = lax.broadcasted_iota(jnp.int32, (members, 1, width), 2)
    mixed = None
    for k in range(ranks):
        feature_hit = (seeds_ref[:, 1:2, k : k + 1] == levels).astype(jnp.float32)
        hidden_hit = (seeds_ref[:, 0:1, k : k + 1] == levels).astype(jnp.float32)
        term = jnp.sum(grouped * feature_hit, axis=2, keepdims=True) * hidden_hit
        mixed = term if mixed is None else mixed + term
    low_ref[:, :width] = (NOISE_SCALE * mixed).reshape(lines, width).astype(low_ref.dtype)
    shift = lax.dot_general(projected, coupling, DIMS, precision=lax.Precision.HIGHEST, preferred_element_type=jnp.float32)
    low_ref[:, width:] = shift.astype(low_ref.dtype)
    right = lax.dot_general(coupling, columns_ref[...].astype(jnp.float32), DIMS, precision=lax.Precision.HIGHEST, preferred_element_type=jnp.float32)
    upper = right.astype(right_ref.dtype)
    right_ref[:width, :] = upper
    right_ref[width:, :] = (right - upper.astype(jnp.float32)).astype(right_ref.dtype)


def lowrank(projected, coupling, seeds, columns):
    lines, width = projected.shape
    depth = columns.shape[0]
    return pl.pallas_call(
        functools.partial(lowrank_kernel, seeds.shape[2]),
        out_shape=[jax.ShapeDtypeStruct((lines, 2 * width), jnp.bfloat16), jax.ShapeDtypeStruct((2 * width, depth), jnp.bfloat16)],
        compiler_params=pltpu.CompilerParams(vmem_limit_bytes=VMEM_LIMIT),
        cost_estimate=pl.CostEstimate(flops=20 * lines * width * width, bytes_accessed=8 * lines * width, transcendentals=0),
        name="lowrank",
    )(projected, coupling, seeds, columns)


def shards(tokens, weight, bank_in, bank_out, fitness, past_seeds, new_seeds):
    members = fitness.shape[0]
    pops, lanes = lax.axis_size("pop"), lax.axis_size("row")
    me, lane = lax.axis_index("pop"), lax.axis_index("row")
    overall = members * pops
    width = bank_out.shape[1]
    features = tokens.shape[2]
    rows, depth = weight.shape
    flat_tokens = tokens.reshape(members * tokens.shape[1], features)
    tile = TILE
    chunks = cut(rows, tile)
    planned = pops == 8 and chunks is not None

    def flip(block, mask):
        return lax.ppermute(block, "pop", [(i, i ^ mask) for i in range(pops)])

    core, one, two = CORE, ONE, TWO

    def send(block, axis):
        return lax.ppermute(block, "pop", [(i, i ^ (axis ^ (one | two) if i & core else axis)) for i in range(pops)])

    packed = jnp.concatenate([fitness[:, None], past_seeds.reshape(members, -1)], axis=1)

    held = {}
    if planned:
        early = take(weight, chunks[1:2])
        late = take(weight, chunks[:1] + chunks[2:])
        own = [late[0], early[0], *late[1:]]
        partner = flip(weight, core)
        for c, piece in enumerate(own):
            held[c, one] = send(piece, one)
            held[c, two] = send(piece, two)
            held[c, one | two] = send(held[c, one], two)
            for mask in (one, two, one | two):
                held[c, mask | core] = flip(held[c, mask], core)
        both = jnp.concatenate([packed, flip(packed, core)], axis=0)
        side = send(both, one)
        across = lax.ppermute(both, "pop", [(i, i ^ (one | two)) for i in range(0, pops, 2)])
        mine = jnp.concatenate([side, across], axis=0)
        theirs = flip(mine, core)
        rest = both.shape[0]
        everyone = jnp.concatenate([both, side, theirs[:rest], across + theirs[rest:]], axis=0)
    else:
        everyone = lax.all_gather(packed, "pop", axis=0, tiled=True)

    every_fitness = everyone[:, 0]
    every_seeds = everyone[:, 1:].reshape((overall,) + past_seeds.shape[1:])
    lower_count = jnp.sum((every_fitness[None, :] < every_fitness[:, None]).astype(jnp.float32), axis=1)
    equal_count = jnp.sum((every_fitness[None, :] == every_fitness[:, None]).astype(jnp.float32), axis=1)
    centered = (lower_count + 0.5 * (equal_count - 1.0)) / (overall - 1.0) - 0.5
    out_hits, in_hits = one_hots(every_seeds, width)
    scaled = (STEP_SCALE * centered)[:, None, None] * out_hits
    coupling = lax.dot_general(
        scaled.reshape(-1, width),
        in_hits.reshape(-1, width),
        (((0,), (0,)), ((), ())),
        precision=lax.Precision.HIGHEST,
    )

    span = bank_in.shape[0]
    banks = [bank_in]
    for step in range(1, lanes):
        banks.append(lax.ppermute(bank_in, "row", [(i, (i - step) % lanes) for i in range(lanes)]))
    if span % depth == 0:
        ring = (lane + jnp.arange(lanes, dtype=jnp.int32)) % lanes
        pick = jnp.concatenate([ring, jnp.stack([me * depth // span, me * depth % span])]).astype(jnp.int32)
        projected, columns = projections(pick, flat_tokens, banks, depth)
    else:
        full_in = jnp.zeros((features, width), bank_in.dtype)
        for step, block in enumerate(banks):
            full_in = lax.dynamic_update_slice_in_dim(full_in, block, ((lane + step) % lanes) * span, 0)
        projected = jnp.dot(flat_tokens, full_in, preferred_element_type=jnp.float32)
        columns = lax.dynamic_slice_in_dim(full_in, me * depth, depth, 0)
    low, right_part = lowrank(projected, coupling, new_seeds, columns)
    new_weight = updated(weight, bank_out, right_part)

    if planned:
        hidden, partial = None, []
        for c, (start, length) in enumerate(chunks):
            near = [(0, weight, start), (core, partner, start)] + [(m, held[c, m], 0) for m in range(2, 6)]
            partial.append(product(flat_tokens, start, length, tile, rows, near, low=low, bank_out=bank_out))
        for c, (start, length) in enumerate(chunks):
            far = [(m, held[c, m], 0) for m in (6, 7)]
            hidden = product(flat_tokens, start, length, tile, rows, far, partial=partial[c], hidden=hidden, resident=c > 1)
    else:
        blocks = {0: weight}
        for bit in range((pops - 1).bit_length()):
            if pops & (pops - 1) == 0:
                blocks.update({m | 1 << bit: flip(b, 1 << bit) for m, b in list(blocks.items())})
        if len(blocks) == pops:
            full = jnp.zeros((rows, features), weight.dtype)
            for m, b in blocks.items():
                full = lax.dynamic_update_slice_in_dim(full, b, (me ^ m) * depth, 1)
        else:
            full = lax.all_gather(weight, "pop", axis=1, tiled=True)
        hidden = lax.dot_general(flat_tokens, full, DIMS, preferred_element_type=jnp.float32)
        hidden += lax.dot_general(low, jnp.concatenate([bank_out, bank_out], axis=1), DIMS, preferred_element_type=jnp.float32)
        hidden = hidden.astype(jnp.bfloat16)
    return (hidden.reshape(members, tokens.shape[1], rows), new_weight)


def solution(mesh):
    placed = (
        P("pop", None, None),
        P("row", "pop"),
        P("row", None),
        P("row", None),
        P("pop"),
        P("pop", None, None),
        P("pop", None, None),
    )
    return jax.shard_map(
        shards,
        mesh=mesh,
        in_specs=placed,
        out_specs=(P("pop", None, "row"), P("row", "pop")),
        check_vma=False,
    )
```

```python
import functools

import jax
import jax.numpy as jnp
from jax import lax
from jax.experimental import pallas as pl
from jax.experimental.pallas import tpu as pltpu
from jax.sharding import PartitionSpec as P


NOISE_SCALE = 0.1
STEP_SCALE = 0.03


def one_hots(seeds, width):
    levels = jnp.arange(width, dtype=jnp.int32)
    out_hits = (seeds[:, 0, :, None] == levels).astype(jnp.float32)
    in_hits = (seeds[:, 1, :, None] == levels).astype(jnp.float32)
    return (out_hits, in_hits)


DIMS = (((1,), (1,)), ((), ()))
TILE = 256
CORE, ONE, TWO = 1, 2, 4
VMEM_LIMIT = 10 * 1024 * 1024


def cut(rows, tile):
    tiles = rows // tile
    if rows % tile or tiles < 8:
        return None
    second = (tiles - 4) * 3 // 10
    lengths = [tiles - 4 - second, second, 2, 2]
    pieces, start = [], 0
    for length in lengths:
        pieces.append((start * tile, length * tile))
        start += length
    return pieces


def source_of(place, me):
    swap = (me ^ place) & CORE
    there = place & CORE
    for axis in (ONE, TWO):
        if place & axis:
            there = there ^ (axis + swap * ((axis ^ ONE ^ TWO) - axis))
    return me ^ there


def product_kernel(places, tile, with_low, with_partial, final, resident, tokens_ref, *refs):
    refs = list(refs)
    out_ref = refs.pop()
    me = lax.axis_index("pop")
    here = pl.ds(pl.multiple_of(pl.program_id(0) * tile, tile), tile)
    total = None
    if with_low:
        low_ref, bank_ref = refs.pop(0), refs.pop(0)
        bank = bank_ref[...]
        total = lax.dot_general(low_ref[...], jnp.concatenate([bank, bank], axis=1), DIMS, preferred_element_type=jnp.float32)
    if with_partial:
        total = refs.pop(0)[:, here]
    for place, block_ref in zip(places, refs):
        depth = block_ref.shape[1]
        columns = pl.ds(pl.multiple_of(source_of(place, me) * depth, 128), depth)
        block = block_ref[here, :] if resident else block_ref[...]
        term = lax.dot_general(tokens_ref[:, columns], block, DIMS, preferred_element_type=jnp.float32)
        total = term if total is None else total + term
    if final:
        out_ref[...] = total.astype(out_ref.dtype)
    else:
        out_ref[:, here] = total


def product(tokens, start, length, tile, rows, blocks, low=None, bank_out=None, partial=None, final=False, hidden=None, resident=False):
    lines = tokens.shape[0]
    base = start // tile
    specs, operands, depth_sum = [pl.BlockSpec(memory_space=pltpu.VMEM)], [tokens], 0

    def add(operand, spec):
        operands.append(operand)
        specs.append(spec)

    if low is not None:
        add(low, pl.BlockSpec(memory_space=pltpu.VMEM))
        add(bank_out, pl.BlockSpec((tile, bank_out.shape[1]), lambda i: (base + i, 0)))
    aliases = {}
    if partial is not None:
        if not final:
            aliases = {len(operands): 0}
        add(partial, pl.BlockSpec(memory_space=pltpu.VMEM))
    for _, block, first in blocks:
        depth = block.shape[1]
        depth_sum += depth
        if resident:
            add(block, pl.BlockSpec(memory_space=pltpu.VMEM))
        else:
            add(block, pl.BlockSpec((tile, depth), functools.partial(lambda i, skip: (skip + i, 0), skip=first // tile)))
    if hidden is not None:
        aliases = {len(operands): 0}
        add(hidden, pl.BlockSpec(memory_space=pl.ANY))
    places = [place for place, _, _ in blocks]

    def kernel(*refs):
        refs = list(refs)
        if hidden is not None:
            refs.pop(-2)
        product_kernel(places, tile, low is not None, partial is not None, final, resident, *refs)

    if final:
        out_shape = jax.ShapeDtypeStruct((lines, rows), jnp.bfloat16)
        out_spec = pl.BlockSpec((lines, tile), lambda i: (0, base + i))
    else:
        out_shape = jax.ShapeDtypeStruct((lines, length), jnp.float32)
        out_spec = pl.BlockSpec(memory_space=pltpu.VMEM)
    return pl.pallas_call(
        kernel,
        grid=(length // tile,),
        in_specs=specs,
        out_specs=out_spec,
        out_shape=out_shape,
        input_output_aliases=aliases,
        compiler_params=pltpu.CompilerParams(vmem_limit_bytes=VMEM_LIMIT),
        cost_estimate=pl.CostEstimate(
            flops=2 * lines * length * depth_sum,
            bytes_accessed=2 * (lines * depth_sum + length * depth_sum + lines * length),
            transcendentals=0,
        ),
    )(*operands)


def take_kernel(pieces, source_ref, *refs):
    outs, sems = refs[: len(pieces)], refs[len(pieces)]
    copies = []
    for (start, length), out in zip(pieces, outs):
        for at in range(0, length, TILE):
            copies.append(pltpu.make_async_copy(source_ref.at[pl.ds(start + at, TILE)], out.at[pl.ds(at, TILE)], sems.at[len(copies)]))
    for copy in copies:
        copy.start()
    for copy in copies:
        copy.wait()


def take(source, pieces):
    depth = source.shape[1]
    size = sum(length for _, length in pieces) * depth * 2
    return pl.pallas_call(
        functools.partial(take_kernel, pieces),
        in_specs=[pl.BlockSpec(memory_space=pl.ANY)],
        out_specs=[pl.BlockSpec(memory_space=pltpu.VMEM)] * len(pieces),
        out_shape=[jax.ShapeDtypeStruct((length, depth), source.dtype) for _, length in pieces],
        scratch_shapes=[pltpu.SemaphoreType.DMA((sum(length for _, length in pieces) // TILE,))],
        compiler_params=pltpu.CompilerParams(vmem_limit_bytes=VMEM_LIMIT),
        cost_estimate=pl.CostEstimate(flops=size, bytes_accessed=2 * size, transcendentals=0),
    )(source)


def update_kernel(weight_ref, bank_ref, right_ref, out_ref):
    bank = bank_ref[...]
    update = jnp.dot(jnp.concatenate([bank, bank], axis=1), right_ref[...], preferred_element_type=jnp.float32)
    out_ref[...] = (weight_ref[...].astype(jnp.float32) + update).astype(out_ref.dtype)


def updated(weight, bank_out, right_part):
    rows, depth = weight.shape
    width = bank_out.shape[1]
    tile = rows // 4 if rows % 64 == 0 else rows
    return pl.pallas_call(
        update_kernel,
        grid=(rows // tile,),
        in_specs=[
            pl.BlockSpec((tile, depth), lambda i: (i, 0)),
            pl.BlockSpec((tile, width), lambda i: (i, 0)),
            pl.BlockSpec(right_part.shape, lambda i: (0, 0)),
        ],
        out_specs=pl.BlockSpec((tile, depth), lambda i: (i, 0)),
        out_shape=jax.ShapeDtypeStruct(weight.shape, weight.dtype),
        compiler_params=pltpu.CompilerParams(vmem_limit_bytes=VMEM_LIMIT),
        cost_estimate=pl.CostEstimate(flops=4 * rows * depth * width, bytes_accessed=4 * rows * depth, transcendentals=0),
        name="update",
    )(weight, bank_out, right_part)


def project_kernel(steps, pick_ref, tokens_ref, *refs):
    blocks, out_ref, columns_ref = refs[:steps], refs[steps], refs[steps + 1]
    total = None
    for j, block_ref in enumerate(blocks):
        span = block_ref.shape[0]
        place = pl.ds(pl.multiple_of(pick_ref[j] * span, 128), span)
        term = jnp.dot(tokens_ref[:, place], block_ref[...], preferred_element_type=jnp.float32)
        total = term if total is None else total + term
    out_ref[...] = total
    depth = columns_ref.shape[0]
    for j, block_ref in enumerate(blocks):

        @pl.when((pl.program_id(0) == 0) & (pick_ref[steps] == pick_ref[j]))
        def _(block_ref=block_ref):
            columns_ref[...] = block_ref[pl.ds(pl.multiple_of(pick_ref[steps + 1], 16), depth), :]


def projections(pick, tokens, blocks, depth):
    lines, features = tokens.shape
    width = blocks[0].shape[1]
    tile = 256 if lines % 256 == 0 else lines
    return pl.pallas_call(
        functools.partial(project_kernel, len(blocks)),
        grid_spec=pltpu.PrefetchScalarGridSpec(
            num_scalar_prefetch=1,
            grid=(lines // tile,),
            in_specs=[pl.BlockSpec((tile, features), lambda i, pick: (i, 0))]
            + [pl.BlockSpec(b.shape, lambda i, pick: (0, 0)) for b in blocks],
            out_specs=[pl.BlockSpec((tile, width), lambda i, pick: (i, 0)), pl.BlockSpec((depth, width), lambda i, pick: (0, 0))],
        ),
        out_shape=[jax.ShapeDtypeStruct((lines, width), jnp.float32), jax.ShapeDtypeStruct((depth, width), blocks[0].dtype)],
        compiler_params=pltpu.CompilerParams(vmem_limit_bytes=VMEM_LIMIT),
        cost_estimate=pl.CostEstimate(flops=2 * lines * features * width, bytes_accessed=2 * lines * features, transcendentals=0),
        name="project",
    )(pick, tokens, *blocks)


def lowrank_kernel(ranks, projected_ref, coupling_ref, seeds_ref, columns_ref, low_ref, right_ref):
    projected, coupling = projected_ref[...], coupling_ref[...]
    members = seeds_ref.shape[0]
    lines, width = projected.shape
    grouped = projected.reshape(members, lines // members, width)
    levels = lax.broadcasted_iota(jnp.int32, (members, 1, width), 2)
    mixed = None
    for k in range(ranks):
        feature_hit = (seeds_ref[:, 1:2, k : k + 1] == levels).astype(jnp.float32)
        hidden_hit = (seeds_ref[:, 0:1, k : k + 1] == levels).astype(jnp.float32)
        term = jnp.sum(grouped * feature_hit, axis=2, keepdims=True) * hidden_hit
        mixed = term if mixed is None else mixed + term
    low_ref[:, :width] = (NOISE_SCALE * mixed).reshape(lines, width).astype(low_ref.dtype)
    shift = lax.dot_general(projected, coupling, DIMS, precision=lax.Precision.HIGHEST, preferred_element_type=jnp.float32)
    low_ref[:, width:] = shift.astype(low_ref.dtype)
    right = lax.dot_general(coupling, columns_ref[...].astype(jnp.float32), DIMS, precision=lax.Precision.HIGHEST, preferred_element_type=jnp.float32)
    upper = right.astype(right_ref.dtype)
    right_ref[:width, :] = upper
    right_ref[width:, :] = (right - upper.astype(jnp.float32)).astype(right_ref.dtype)


def lowrank(projected, coupling, seeds, columns):
    lines, width = projected.shape
    depth = columns.shape[0]
    return pl.pallas_call(
        functools.partial(lowrank_kernel, seeds.shape[2]),
        out_shape=[jax.ShapeDtypeStruct((lines, 2 * width), jnp.bfloat16), jax.ShapeDtypeStruct((2 * width, depth), jnp.bfloat16)],
        compiler_params=pltpu.CompilerParams(vmem_limit_bytes=VMEM_LIMIT),
        cost_estimate=pl.CostEstimate(flops=20 * lines * width * width, bytes_accessed=8 * lines * width, transcendentals=0),
        name="lowrank",
    )(projected, coupling, seeds, columns)


def shards(tokens, weight, bank_in, bank_out, fitness, past_seeds, new_seeds):
    members = fitness.shape[0]
    pops, lanes = lax.axis_size("pop"), lax.axis_size("row")
    me, lane = lax.axis_index("pop"), lax.axis_index("row")
    overall = members * pops
    width = bank_out.shape[1]
    features = tokens.shape[2]
    rows, depth = weight.shape
    flat_tokens = tokens.reshape(members * tokens.shape[1], features)
    tile = TILE
    chunks = cut(rows, tile)
    planned = pops == 8 and chunks is not None

    def flip(block, mask):
        return lax.ppermute(block, "pop", [(i, i ^ mask) for i in range(pops)])

    core, one, two = CORE, ONE, TWO

    def send(block, axis):
        return lax.ppermute(block, "pop", [(i, i ^ (axis ^ (one | two) if i & core else axis)) for i in range(pops)])

    packed = jnp.concatenate([fitness[:, None], past_seeds.reshape(members, -1)], axis=1)

    held = {}
    if planned:
        held[two] = send(weight, two)
        early = take(weight, chunks[1:2])
        late = take(weight, chunks[:1] + chunks[2:])
        own = [late[0], early[0], *late[1:]]
        partner = flip(weight, core)
        held[two | core] = flip(held[two], core)
        for c, piece in enumerate(own):
            held[c, one] = send(piece, one)
            held[c, one | two] = send(held[c, one], two)
            for mask in (one, one | two):
                held[c, mask | core] = flip(held[c, mask], core)
        both = jnp.concatenate([packed, flip(packed, core)], axis=0)
        side = send(both, one)
        across = lax.ppermute(both, "pop", [(i, i ^ (one | two)) for i in range(0, pops, 2)])
        mine = jnp.concatenate([side, across], axis=0)
        theirs = flip(mine, core)
        rest = both.shape[0]
        everyone = jnp.concatenate([both, side, theirs[:rest], across + theirs[rest:]], axis=0)
    else:
        everyone = lax.all_gather(packed, "pop", axis=0, tiled=True)

    every_fitness = everyone[:, 0]
    every_seeds = everyone[:, 1:].reshape((overall,) + past_seeds.shape[1:])
    lower_count = jnp.sum((every_fitness[None, :] < every_fitness[:, None]).astype(jnp.float32), axis=1)
    equal_count = jnp.sum((every_fitness[None, :] == every_fitness[:, None]).astype(jnp.float32), axis=1)
    centered = (lower_count + 0.5 * (equal_count - 1.0)) / (overall - 1.0) - 0.5
    out_hits, in_hits = one_hots(every_seeds, width)
    scaled = (STEP_SCALE * centered)[:, None, None] * out_hits
    coupling = lax.dot_general(
        scaled.reshape(-1, width),
        in_hits.reshape(-1, width),
        (((0,), (0,)), ((), ())),
        precision=lax.Precision.HIGHEST,
    )

    span = bank_in.shape[0]
    banks = [bank_in]
    for step in range(1, lanes):
        banks.append(lax.ppermute(bank_in, "row", [(i, (i - step) % lanes) for i in range(lanes)]))
    if span % depth == 0:
        ring = (lane + jnp.arange(lanes, dtype=jnp.int32)) % lanes
        pick = jnp.concatenate([ring, jnp.stack([me * depth // span, me * depth % span])]).astype(jnp.int32)
        projected, columns = projections(pick, flat_tokens, banks, depth)
    else:
        full_in = jnp.zeros((features, width), bank_in.dtype)
        for step, block in enumerate(banks):
            full_in = lax.dynamic_update_slice_in_dim(full_in, block, ((lane + step) % lanes) * span, 0)
        projected = jnp.dot(flat_tokens, full_in, preferred_element_type=jnp.float32)
        columns = lax.dynamic_slice_in_dim(full_in, me * depth, depth, 0)
    low, right_part = lowrank(projected, coupling, new_seeds, columns)
    new_weight = updated(weight, bank_out, right_part)

    if planned:
        hidden, partial = None, []
        for c, (start, length) in enumerate(chunks):
            near = [(0, weight, start), (core, partner, start)] + [(m, held[c, m], 0) for m in (one, one | core)]
            part = product(flat_tokens, start, length, tile, rows, near, low=low, bank_out=bank_out)
            side = [(m, held[m], start) for m in (two, two | core)]
            partial.append(product(flat_tokens, start, length, tile, rows, side, partial=part))
        for c, (start, length) in enumerate(chunks):
            far = [(m, held[c, m], 0) for m in (6, 7)]
            hidden = product(flat_tokens, start, length, tile, rows, far, partial=partial[c], final=True, hidden=hidden, resident=c > 1)
    else:
        blocks = {0: weight}
        for bit in range((pops - 1).bit_length()):
            if pops & (pops - 1) == 0:
                blocks.update({m | 1 << bit: flip(b, 1 << bit) for m, b in list(blocks.items())})
        if len(blocks) == pops:
            full = jnp.zeros((rows, features), weight.dtype)
            for m, b in blocks.items():
                full = lax.dynamic_update_slice_in_dim(full, b, (me ^ m) * depth, 1)
        else:
            full = lax.all_gather(weight, "pop", axis=1, tiled=True)
        hidden = lax.dot_general(flat_tokens, full, DIMS, preferred_element_type=jnp.float32)
        hidden += lax.dot_general(low, jnp.concatenate([bank_out, bank_out], axis=1), DIMS, preferred_element_type=jnp.float32)
        hidden = hidden.astype(jnp.bfloat16)
    return (hidden.reshape(members, tokens.shape[1], rows), new_weight)


def solution(mesh):
    placed = (
        P("pop", None, None),
        P("row", "pop"),
        P("row", None),
        P("row", None),
        P("pop"),
        P("pop", None, None),
        P("pop", None, None),
    )
    return jax.shard_map(
        shards,
        mesh=mesh,
        in_specs=placed,
        out_specs=(P("pop", None, "row"), P("row", "pop")),
        check_vma=False,
    )
```

```python
import functools

import jax
import jax.numpy as jnp
from jax import lax
from jax.experimental import pallas as pl
from jax.experimental.pallas import tpu as pltpu
from jax.sharding import PartitionSpec as P


NOISE_SCALE = 0.1
STEP_SCALE = 0.03


def one_hots(seeds, width):
    levels = jnp.arange(width, dtype=jnp.int32)
    out_hits = (seeds[:, 0, :, None] == levels).astype(jnp.float32)
    in_hits = (seeds[:, 1, :, None] == levels).astype(jnp.float32)
    return (out_hits, in_hits)


DIMS = (((1,), (1,)), ((), ()))
TILE = 256
CORE, ONE, TWO = 1, 2, 4
VMEM_LIMIT = 10 * 1024 * 1024


def cut(rows, tile):
    tiles = rows // tile
    if rows % tile or tiles < 8:
        return None
    second = (tiles - 4) * 3 // 10
    lengths = [tiles - 4 - second, second, 2, 2]
    pieces, start = [], 0
    for length in lengths:
        pieces.append((start * tile, length * tile))
        start += length
    return pieces


def source_of(place, me):
    swap = (me ^ place) & CORE
    there = place & CORE
    for axis in (ONE, TWO):
        if place & axis:
            there = there ^ (axis + swap * ((axis ^ ONE ^ TWO) - axis))
    return me ^ there


def product_kernel(places, tile, with_low, with_partial, final, resident, tokens_ref, *refs):
    refs = list(refs)
    out_ref = refs.pop()
    me = lax.axis_index("pop")
    here = pl.ds(pl.multiple_of(pl.program_id(0) * tile, tile), tile)
    total = None
    if with_low:
        low_ref, bank_ref = refs.pop(0), refs.pop(0)
        bank = bank_ref[...]
        total = lax.dot_general(low_ref[...], jnp.concatenate([bank, bank], axis=1), DIMS, preferred_element_type=jnp.float32)
    if with_partial:
        total = refs.pop(0)[:, here]
    for place, block_ref in zip(places, refs):
        depth = block_ref.shape[1]
        columns = pl.ds(pl.multiple_of(source_of(place, me) * depth, 128), depth)
        block = block_ref[here, :] if resident else block_ref[...]
        term = lax.dot_general(tokens_ref[:, columns], block, DIMS, preferred_element_type=jnp.float32)
        total = term if total is None else total + term
    if final:
        out_ref[...] = total.astype(out_ref.dtype)
    else:
        out_ref[:, here] = total


def product(tokens, start, length, tile, rows, blocks, low=None, bank_out=None, partial=None, final=False, hidden=None, resident=False):
    lines = tokens.shape[0]
    base = start // tile
    specs, operands, depth_sum = [pl.BlockSpec(memory_space=pltpu.VMEM)], [tokens], 0

    def add(operand, spec):
        operands.append(operand)
        specs.append(spec)

    if low is not None:
        add(low, pl.BlockSpec(memory_space=pltpu.VMEM))
        add(bank_out, pl.BlockSpec((tile, bank_out.shape[1]), lambda i: (base + i, 0)))
    aliases = {}
    if partial is not None:
        if not final:
            aliases = {len(operands): 0}
        add(partial, pl.BlockSpec(memory_space=pltpu.VMEM))
    for _, block, first in blocks:
        depth = block.shape[1]
        depth_sum += depth
        if resident:
            add(block, pl.BlockSpec(memory_space=pltpu.VMEM))
        else:
            add(block, pl.BlockSpec((tile, depth), functools.partial(lambda i, skip: (skip + i, 0), skip=first // tile)))
    if hidden is not None:
        aliases = {len(operands): 0}
        add(hidden, pl.BlockSpec(memory_space=pl.ANY))
    places = [place for place, _, _ in blocks]

    def kernel(*refs):
        refs = list(refs)
        if hidden is not None:
            refs.pop(-2)
        product_kernel(places, tile, low is not None, partial is not None, final, resident, *refs)

    if final:
        out_shape = jax.ShapeDtypeStruct((lines, rows), jnp.bfloat16)
        out_spec = pl.BlockSpec((lines, tile), lambda i: (0, base + i))
    else:
        out_shape = jax.ShapeDtypeStruct((lines, length), jnp.float32)
        out_spec = pl.BlockSpec(memory_space=pltpu.VMEM)
    return pl.pallas_call(
        kernel,
        grid=(length // tile,),
        in_specs=specs,
        out_specs=out_spec,
        out_shape=out_shape,
        input_output_aliases=aliases,
        compiler_params=pltpu.CompilerParams(vmem_limit_bytes=VMEM_LIMIT),
        cost_estimate=pl.CostEstimate(
            flops=2 * lines * length * depth_sum,
            bytes_accessed=2 * (lines * depth_sum + length * depth_sum + lines * length),
            transcendentals=0,
        ),
    )(*operands)


def take_kernel(pieces, source_ref, *refs):
    outs, sems = refs[: len(pieces)], refs[len(pieces)]
    copies = []
    for (start, length), out in zip(pieces, outs):
        for at in range(0, length, TILE):
            copies.append(pltpu.make_async_copy(source_ref.at[pl.ds(start + at, TILE)], out.at[pl.ds(at, TILE)], sems.at[len(copies)]))
    for copy in copies:
        copy.start()
    for copy in copies:
        copy.wait()


def take(source, pieces):
    depth = source.shape[1]
    size = sum(length for _, length in pieces) * depth * 2
    return pl.pallas_call(
        functools.partial(take_kernel, pieces),
        in_specs=[pl.BlockSpec(memory_space=pl.ANY)],
        out_specs=[pl.BlockSpec(memory_space=pltpu.VMEM)] * len(pieces),
        out_shape=[jax.ShapeDtypeStruct((length, depth), source.dtype) for _, length in pieces],
        scratch_shapes=[pltpu.SemaphoreType.DMA((sum(length for _, length in pieces) // TILE,))],
        compiler_params=pltpu.CompilerParams(vmem_limit_bytes=VMEM_LIMIT),
        cost_estimate=pl.CostEstimate(flops=size, bytes_accessed=2 * size, transcendentals=0),
    )(source)


def update_kernel(weight_ref, bank_ref, right_ref, out_ref):
    bank = bank_ref[...]
    update = jnp.dot(jnp.concatenate([bank, bank], axis=1), right_ref[...], preferred_element_type=jnp.float32)
    out_ref[...] = (weight_ref[...].astype(jnp.float32) + update).astype(out_ref.dtype)


def updated(weight, bank_out, right_part):
    rows, depth = weight.shape
    width = bank_out.shape[1]
    tile = rows // 4 if rows % 64 == 0 else rows
    return pl.pallas_call(
        update_kernel,
        grid=(rows // tile,),
        in_specs=[
            pl.BlockSpec((tile, depth), lambda i: (i, 0)),
            pl.BlockSpec((tile, width), lambda i: (i, 0)),
            pl.BlockSpec(right_part.shape, lambda i: (0, 0)),
        ],
        out_specs=pl.BlockSpec((tile, depth), lambda i: (i, 0)),
        out_shape=jax.ShapeDtypeStruct(weight.shape, weight.dtype),
        compiler_params=pltpu.CompilerParams(vmem_limit_bytes=VMEM_LIMIT),
        cost_estimate=pl.CostEstimate(flops=4 * rows * depth * width, bytes_accessed=4 * rows * depth, transcendentals=0),
        name="update",
    )(weight, bank_out, right_part)


def project_kernel(steps, pick_ref, tokens_ref, *refs):
    blocks, out_ref, columns_ref = refs[:steps], refs[steps], refs[steps + 1]
    total = None
    for j, block_ref in enumerate(blocks):
        span = block_ref.shape[0]
        place = pl.ds(pl.multiple_of(pick_ref[j] * span, 128), span)
        term = jnp.dot(tokens_ref[:, place], block_ref[...], preferred_element_type=jnp.float32)
        total = term if total is None else total + term
    out_ref[...] = total
    depth = columns_ref.shape[0]
    for j, block_ref in enumerate(blocks):

        @pl.when((pl.program_id(0) == 0) & (pick_ref[steps] == pick_ref[j]))
        def _(block_ref=block_ref):
            columns_ref[...] = block_ref[pl.ds(pl.multiple_of(pick_ref[steps + 1], 16), depth), :]


def projections(pick, tokens, blocks, depth):
    lines, features = tokens.shape
    width = blocks[0].shape[1]
    tile = 256 if lines % 256 == 0 else lines
    return pl.pallas_call(
        functools.partial(project_kernel, len(blocks)),
        grid_spec=pltpu.PrefetchScalarGridSpec(
            num_scalar_prefetch=1,
            grid=(lines // tile,),
            in_specs=[pl.BlockSpec((tile, features), lambda i, pick: (i, 0))]
            + [pl.BlockSpec(b.shape, lambda i, pick: (0, 0)) for b in blocks],
            out_specs=[pl.BlockSpec((tile, width), lambda i, pick: (i, 0)), pl.BlockSpec((depth, width), lambda i, pick: (0, 0))],
        ),
        out_shape=[jax.ShapeDtypeStruct((lines, width), jnp.float32), jax.ShapeDtypeStruct((depth, width), blocks[0].dtype)],
        compiler_params=pltpu.CompilerParams(vmem_limit_bytes=VMEM_LIMIT),
        cost_estimate=pl.CostEstimate(flops=2 * lines * features * width, bytes_accessed=2 * lines * features, transcendentals=0),
        name="project",
    )(pick, tokens, *blocks)


def lowrank_kernel(ranks, projected_ref, coupling_ref, seeds_ref, columns_ref, low_ref, right_ref):
    projected, coupling = projected_ref[...], coupling_ref[...]
    members = seeds_ref.shape[0]
    lines, width = projected.shape
    grouped = projected.reshape(members, lines // members, width)
    levels = lax.broadcasted_iota(jnp.int32, (members, 1, width), 2)
    mixed = None
    for k in range(ranks):
        feature_hit = (seeds_ref[:, 1:2, k : k + 1] == levels).astype(jnp.float32)
        hidden_hit = (seeds_ref[:, 0:1, k : k + 1] == levels).astype(jnp.float32)
        term = jnp.sum(grouped * feature_hit, axis=2, keepdims=True) * hidden_hit
        mixed = term if mixed is None else mixed + term
    low_ref[:, :width] = (NOISE_SCALE * mixed).reshape(lines, width).astype(low_ref.dtype)
    shift = lax.dot_general(projected, coupling, DIMS, precision=lax.Precision.HIGHEST, preferred_element_type=jnp.float32)
    low_ref[:, width:] = shift.astype(low_ref.dtype)
    right = lax.dot_general(coupling, columns_ref[...].astype(jnp.float32), DIMS, precision=lax.Precision.HIGHEST, preferred_element_type=jnp.float32)
    upper = right.astype(right_ref.dtype)
    right_ref[:width, :] = upper
    right_ref[width:, :] = (right - upper.astype(jnp.float32)).astype(right_ref.dtype)


def lowrank(projected, coupling, seeds, columns):
    lines, width = projected.shape
    depth = columns.shape[0]
    return pl.pallas_call(
        functools.partial(lowrank_kernel, seeds.shape[2]),
        out_shape=[jax.ShapeDtypeStruct((lines, 2 * width), jnp.bfloat16), jax.ShapeDtypeStruct((2 * width, depth), jnp.bfloat16)],
        compiler_params=pltpu.CompilerParams(vmem_limit_bytes=VMEM_LIMIT),
        cost_estimate=pl.CostEstimate(flops=20 * lines * width * width, bytes_accessed=8 * lines * width, transcendentals=0),
        name="lowrank",
    )(projected, coupling, seeds, columns)


def shards(tokens, weight, bank_in, bank_out, fitness, past_seeds, new_seeds):
    members = fitness.shape[0]
    pops, lanes = lax.axis_size("pop"), lax.axis_size("row")
    me, lane = lax.axis_index("pop"), lax.axis_index("row")
    overall = members * pops
    width = bank_out.shape[1]
    features = tokens.shape[2]
    rows, depth = weight.shape
    flat_tokens = tokens.reshape(members * tokens.shape[1], features)
    tile = TILE
    chunks = cut(rows, tile)
    planned = pops == 8 and chunks is not None

    def flip(block, mask):
        return lax.ppermute(block, "pop", [(i, i ^ mask) for i in range(pops)])

    core, one, two = CORE, ONE, TWO

    def send(block, axis):
        return lax.ppermute(block, "pop", [(i, i ^ (axis ^ (one | two) if i & core else axis)) for i in range(pops)])

    packed = jnp.concatenate([fitness[:, None], past_seeds.reshape(members, -1)], axis=1)

    held = {}
    if planned:
        held[two] = send(weight, two)
        early = take(weight, chunks[1:2])
        late = take(weight, chunks[:1] + chunks[2:])
        own = [late[0], early[0], *late[1:]]
        partner = flip(weight, core)
        held[two | core] = flip(held[two], core)
        for c, piece in enumerate(own):
            held[c, one] = send(piece, one)
            held[c, one | two] = send(held[c, one], two)
            for mask in (one, one | two):
                held[c, mask | core] = flip(held[c, mask], core)
        both = jnp.concatenate([packed, flip(packed, core)], axis=0)
        side = send(both, one)
        across = lax.ppermute(both, "pop", [(i, i ^ (one | two)) for i in range(0, pops, 2)])
        mine = jnp.concatenate([side, across], axis=0)
        theirs = flip(mine, core)
        rest = both.shape[0]
        everyone = jnp.concatenate([both, side, theirs[:rest], across + theirs[rest:]], axis=0)
    else:
        everyone = lax.all_gather(packed, "pop", axis=0, tiled=True)

    every_fitness = everyone[:, 0]
    every_seeds = everyone[:, 1:].reshape((overall,) + past_seeds.shape[1:])
    lower_count = jnp.sum((every_fitness[None, :] < every_fitness[:, None]).astype(jnp.float32), axis=1)
    equal_count = jnp.sum((every_fitness[None, :] == every_fitness[:, None]).astype(jnp.float32), axis=1)
    centered = (lower_count + 0.5 * (equal_count - 1.0)) / (overall - 1.0) - 0.5
    out_hits, in_hits = one_hots(every_seeds, width)
    scaled = (STEP_SCALE * centered)[:, None, None] * out_hits
    coupling = lax.dot_general(
        scaled.reshape(-1, width),
        in_hits.reshape(-1, width),
        (((0,), (0,)), ((), ())),
        precision=lax.Precision.HIGHEST,
    )

    span = bank_in.shape[0]
    banks = [bank_in]
    for step in range(1, lanes):
        banks.append(lax.ppermute(bank_in, "row", [(i, (i - step) % lanes) for i in range(lanes)]))
    if span % depth == 0:
        ring = (lane + jnp.arange(lanes, dtype=jnp.int32)) % lanes
        pick = jnp.concatenate([ring, jnp.stack([me * depth // span, me * depth % span])]).astype(jnp.int32)
        projected, columns = projections(pick, flat_tokens, banks, depth)
    else:
        full_in = jnp.zeros((features, width), bank_in.dtype)
        for step, block in enumerate(banks):
            full_in = lax.dynamic_update_slice_in_dim(full_in, block, ((lane + step) % lanes) * span, 0)
        projected = jnp.dot(flat_tokens, full_in, preferred_element_type=jnp.float32)
        columns = lax.dynamic_slice_in_dim(full_in, me * depth, depth, 0)
    low, right_part = lowrank(projected, coupling, new_seeds, columns)
    new_weight = updated(weight, bank_out, right_part)

    if planned:
        hidden, partial = None, []
        for c, (start, length) in enumerate(chunks):
            near = [(0, weight, start), (core, partner, start)] + [(m, held[c, m], 0) for m in (one, one | core)]
            part = product(flat_tokens, start, length, tile, rows, near, low=low, bank_out=bank_out)
            side = [(m, held[m], start) for m in (two, two | core)]
            partial.append(product(flat_tokens, start, length, tile, rows, side, partial=part))
        for c, (start, length) in enumerate(chunks):
            far = [(m, held[c, m], 0) for m in (6, 7)]
            if c + 1 == len(chunks):
                partial[c] = product(flat_tokens, start, length, tile, rows, far[:1], partial=partial[c], resident=True)
                far = far[1:]
            hidden = product(flat_tokens, start, length, length if c > 1 and start % length == 0 else tile, rows, far, partial=partial[c], final=True, hidden=hidden, resident=c > 1)
    else:
        blocks = {0: weight}
        for bit in range((pops - 1).bit_length()):
            if pops & (pops - 1) == 0:
                blocks.update({m | 1 << bit: flip(b, 1 << bit) for m, b in list(blocks.items())})
        if len(blocks) == pops:
            full = jnp.zeros((rows, features), weight.dtype)
            for m, b in blocks.items():
                full = lax.dynamic_update_slice_in_dim(full, b, (me ^ m) * depth, 1)
        else:
            full = lax.all_gather(weight, "pop", axis=1, tiled=True)
        hidden = lax.dot_general(flat_tokens, full, DIMS, preferred_element_type=jnp.float32)
        hidden += lax.dot_general(low, jnp.concatenate([bank_out, bank_out], axis=1), DIMS, preferred_element_type=jnp.float32)
        hidden = hidden.astype(jnp.bfloat16)
    return (hidden.reshape(members, tokens.shape[1], rows), new_weight)


def solution(mesh):
    placed = (
        P("pop", None, None),
        P("row", "pop"),
        P("row", None),
        P("row", None),
        P("pop"),
        P("pop", None, None),
        P("pop", None, None),
    )
    return jax.shard_map(
        shards,
        mesh=mesh,
        in_specs=placed,
        out_specs=(P("pop", None, "row"), P("row", "pop")),
        check_vma=False,
    )
```

```python
import functools

import jax
import jax.numpy as jnp
from jax import lax
from jax.experimental import pallas as pl
from jax.experimental.pallas import tpu as pltpu
from jax.sharding import PartitionSpec as P


NOISE_SCALE = 0.1
STEP_SCALE = 0.03


def one_hots(seeds, width):
    levels = jnp.arange(width, dtype=jnp.int32)
    out_hits = (seeds[:, 0, :, None] == levels).astype(jnp.float32)
    in_hits = (seeds[:, 1, :, None] == levels).astype(jnp.float32)
    return (out_hits, in_hits)


DIMS = (((1,), (1,)), ((), ()))
TILE = 256
CORE, ONE, TWO = 1, 2, 4
VMEM_LIMIT = 10 * 1024 * 1024


def cut(rows, tile):
    tiles = rows // tile
    if rows % tile or tiles < 8:
        return None
    second = (tiles - 3) * 2 // 5
    lengths = [tiles - 3 - second, second, 2, 1]
    pieces, start = [], 0
    for length in lengths:
        pieces.append((start * tile, length * tile))
        start += length
    return pieces


def source_of(place, me):
    swap = (me ^ place) & CORE
    there = place & CORE
    for axis in (ONE, TWO):
        if place & axis:
            there = there ^ (axis + swap * ((axis ^ ONE ^ TWO) - axis))
    return me ^ there


def product_kernel(places, tile, with_low, with_partial, final, resident, tokens_ref, *refs):
    refs = list(refs)
    out_ref = refs.pop()
    me = lax.axis_index("pop")
    here = pl.ds(pl.multiple_of(pl.program_id(0) * tile, tile), tile)
    total = None
    if with_low:
        low_ref, bank_ref = refs.pop(0), refs.pop(0)
        bank = bank_ref[...]
        total = lax.dot_general(low_ref[...], jnp.concatenate([bank, bank], axis=1), DIMS, preferred_element_type=jnp.float32)
    if with_partial:
        total = refs.pop(0)[:, here]
    for place, block_ref in zip(places, refs):
        depth = block_ref.shape[1]
        columns = pl.ds(pl.multiple_of(source_of(place, me) * depth, 128), depth)
        block = block_ref[here, :] if resident else block_ref[...]
        term = lax.dot_general(tokens_ref[:, columns], block, DIMS, preferred_element_type=jnp.float32)
        total = term if total is None else total + term
    if final:
        out_ref[...] = total.astype(out_ref.dtype)
    else:
        out_ref[:, here] = total


def product(tokens, start, length, tile, rows, blocks, low=None, bank_out=None, partial=None, final=False, hidden=None, resident=False):
    lines = tokens.shape[0]
    base = start // tile
    specs, operands, depth_sum = [pl.BlockSpec(memory_space=pltpu.VMEM)], [tokens], 0

    def add(operand, spec):
        operands.append(operand)
        specs.append(spec)

    if low is not None:
        add(low, pl.BlockSpec(memory_space=pltpu.VMEM))
        add(bank_out, pl.BlockSpec((tile, bank_out.shape[1]), lambda i: (base + i, 0)))
    aliases = {}
    if partial is not None:
        if not final:
            aliases = {len(operands): 0}
        add(partial, pl.BlockSpec(memory_space=pltpu.VMEM))
    for _, block, first in blocks:
        depth = block.shape[1]
        depth_sum += depth
        if resident:
            add(block, pl.BlockSpec(memory_space=pltpu.VMEM))
        else:
            add(block, pl.BlockSpec((tile, depth), functools.partial(lambda i, skip: (skip + i, 0), skip=first // tile)))
    if hidden is not None:
        aliases = {len(operands): 0}
        add(hidden, pl.BlockSpec(memory_space=pl.ANY))
    places = [place for place, _, _ in blocks]

    def kernel(*refs):
        refs = list(refs)
        if hidden is not None:
            refs.pop(-2)
        product_kernel(places, tile, low is not None, partial is not None, final, resident, *refs)

    if final:
        out_shape = jax.ShapeDtypeStruct((lines, rows), jnp.bfloat16)
        out_spec = pl.BlockSpec((lines, tile), lambda i: (0, base + i))
    else:
        out_shape = jax.ShapeDtypeStruct((lines, length), jnp.float32)
        out_spec = pl.BlockSpec(memory_space=pltpu.VMEM)
    return pl.pallas_call(
        kernel,
        grid=(length // tile,),
        in_specs=specs,
        out_specs=out_spec,
        out_shape=out_shape,
        input_output_aliases=aliases,
        compiler_params=pltpu.CompilerParams(vmem_limit_bytes=VMEM_LIMIT),
        cost_estimate=pl.CostEstimate(
            flops=2 * lines * length * depth_sum,
            bytes_accessed=2 * (lines * depth_sum + length * depth_sum + lines * length),
            transcendentals=0,
        ),
    )(*operands)


def take_kernel(pieces, source_ref, *refs):
    outs, sems = refs[: len(pieces)], refs[len(pieces)]
    copies = []
    for (start, length), out in zip(pieces, outs):
        for at in range(0, length, TILE):
            copies.append(pltpu.make_async_copy(source_ref.at[pl.ds(start + at, TILE)], out.at[pl.ds(at, TILE)], sems.at[len(copies)]))
    for copy in copies:
        copy.start()
    for copy in copies:
        copy.wait()


def take(source, pieces):
    depth = source.shape[1]
    size = sum(length for _, length in pieces) * depth * 2
    return pl.pallas_call(
        functools.partial(take_kernel, pieces),
        in_specs=[pl.BlockSpec(memory_space=pl.ANY)],
        out_specs=[pl.BlockSpec(memory_space=pltpu.VMEM)] * len(pieces),
        out_shape=[jax.ShapeDtypeStruct((length, depth), source.dtype) for _, length in pieces],
        scratch_shapes=[pltpu.SemaphoreType.DMA((sum(length for _, length in pieces) // TILE,))],
        compiler_params=pltpu.CompilerParams(vmem_limit_bytes=VMEM_LIMIT),
        cost_estimate=pl.CostEstimate(flops=size, bytes_accessed=2 * size, transcendentals=0),
    )(source)


def update_kernel(weight_ref, bank_ref, right_ref, out_ref):
    bank = bank_ref[...]
    update = jnp.dot(jnp.concatenate([bank, bank], axis=1), right_ref[...], preferred_element_type=jnp.float32)
    out_ref[...] = (weight_ref[...].astype(jnp.float32) + update).astype(out_ref.dtype)


def updated(weight, bank_out, right_part):
    rows, depth = weight.shape
    width = bank_out.shape[1]
    tile = rows // 4 if rows % 64 == 0 else rows
    return pl.pallas_call(
        update_kernel,
        grid=(rows // tile,),
        in_specs=[
            pl.BlockSpec((tile, depth), lambda i: (i, 0)),
            pl.BlockSpec((tile, width), lambda i: (i, 0)),
            pl.BlockSpec(right_part.shape, lambda i: (0, 0)),
        ],
        out_specs=pl.BlockSpec((tile, depth), lambda i: (i, 0)),
        out_shape=jax.ShapeDtypeStruct(weight.shape, weight.dtype),
        compiler_params=pltpu.CompilerParams(vmem_limit_bytes=VMEM_LIMIT),
        cost_estimate=pl.CostEstimate(flops=4 * rows * depth * width, bytes_accessed=4 * rows * depth, transcendentals=0),
        name="update",
    )(weight, bank_out, right_part)


def project_kernel(steps, pick_ref, tokens_ref, *refs):
    blocks, out_ref, columns_ref = refs[:steps], refs[steps], refs[steps + 1]
    total = None
    for j, block_ref in enumerate(blocks):
        span = block_ref.shape[0]
        place = pl.ds(pl.multiple_of(pick_ref[j] * span, 128), span)
        term = jnp.dot(tokens_ref[:, place], block_ref[...], preferred_element_type=jnp.float32)
        total = term if total is None else total + term
    out_ref[...] = total
    depth = columns_ref.shape[0]
    for j, block_ref in enumerate(blocks):

        @pl.when((pl.program_id(0) == 0) & (pick_ref[steps] == pick_ref[j]))
        def _(block_ref=block_ref):
            columns_ref[...] = block_ref[pl.ds(pl.multiple_of(pick_ref[steps + 1], 16), depth), :]


def projections(pick, tokens, blocks, depth):
    lines, features = tokens.shape
    width = blocks[0].shape[1]
    tile = 256 if lines % 256 == 0 else lines
    return pl.pallas_call(
        functools.partial(project_kernel, len(blocks)),
        grid_spec=pltpu.PrefetchScalarGridSpec(
            num_scalar_prefetch=1,
            grid=(lines // tile,),
            in_specs=[pl.BlockSpec((tile, features), lambda i, pick: (i, 0))]
            + [pl.BlockSpec(b.shape, lambda i, pick: (0, 0)) for b in blocks],
            out_specs=[pl.BlockSpec((tile, width), lambda i, pick: (i, 0)), pl.BlockSpec((depth, width), lambda i, pick: (0, 0))],
        ),
        out_shape=[jax.ShapeDtypeStruct((lines, width), jnp.float32), jax.ShapeDtypeStruct((depth, width), blocks[0].dtype)],
        compiler_params=pltpu.CompilerParams(vmem_limit_bytes=VMEM_LIMIT),
        cost_estimate=pl.CostEstimate(flops=2 * lines * features * width, bytes_accessed=2 * lines * features, transcendentals=0),
        name="project",
    )(pick, tokens, *blocks)


def lowrank_kernel(ranks, projected_ref, coupling_ref, seeds_ref, columns_ref, low_ref, right_ref):
    projected, coupling = projected_ref[...], coupling_ref[...]
    members = seeds_ref.shape[0]
    lines, width = projected.shape
    grouped = projected.reshape(members, lines // members, width)
    levels = lax.broadcasted_iota(jnp.int32, (members, 1, width), 2)
    mixed = None
    for k in range(ranks):
        feature_hit = (seeds_ref[:, 1:2, k : k + 1] == levels).astype(jnp.float32)
        hidden_hit = (seeds_ref[:, 0:1, k : k + 1] == levels).astype(jnp.float32)
        term = jnp.sum(grouped * feature_hit, axis=2, keepdims=True) * hidden_hit
        mixed = term if mixed is None else mixed + term
    low_ref[:, :width] = (NOISE_SCALE * mixed).reshape(lines, width).astype(low_ref.dtype)
    shift = lax.dot_general(projected, coupling, DIMS, precision=lax.Precision.HIGHEST, preferred_element_type=jnp.float32)
    low_ref[:, width:] = shift.astype(low_ref.dtype)
    right = lax.dot_general(coupling, columns_ref[...].astype(jnp.float32), DIMS, precision=lax.Precision.HIGHEST, preferred_element_type=jnp.float32)
    upper = right.astype(right_ref.dtype)
    right_ref[:width, :] = upper
    right_ref[width:, :] = (right - upper.astype(jnp.float32)).astype(right_ref.dtype)


def lowrank(projected, coupling, seeds, columns):
    lines, width = projected.shape
    depth = columns.shape[0]
    return pl.pallas_call(
        functools.partial(lowrank_kernel, seeds.shape[2]),
        out_shape=[jax.ShapeDtypeStruct((lines, 2 * width), jnp.bfloat16), jax.ShapeDtypeStruct((2 * width, depth), jnp.bfloat16)],
        compiler_params=pltpu.CompilerParams(vmem_limit_bytes=VMEM_LIMIT),
        cost_estimate=pl.CostEstimate(flops=20 * lines * width * width, bytes_accessed=8 * lines * width, transcendentals=0),
        name="lowrank",
    )(projected, coupling, seeds, columns)


def shards(tokens, weight, bank_in, bank_out, fitness, past_seeds, new_seeds):
    members = fitness.shape[0]
    pops, lanes = lax.axis_size("pop"), lax.axis_size("row")
    me, lane = lax.axis_index("pop"), lax.axis_index("row")
    overall = members * pops
    width = bank_out.shape[1]
    features = tokens.shape[2]
    rows, depth = weight.shape
    flat_tokens = tokens.reshape(members * tokens.shape[1], features)
    tile = TILE
    chunks = cut(rows, tile)
    planned = pops == 8 and chunks is not None

    def flip(block, mask):
        return lax.ppermute(block, "pop", [(i, i ^ mask) for i in range(pops)])

    core, one, two = CORE, ONE, TWO

    def send(block, axis):
        return lax.ppermute(block, "pop", [(i, i ^ (axis ^ (one | two) if i & core else axis)) for i in range(pops)])

    packed = jnp.concatenate([fitness[:, None], past_seeds.reshape(members, -1)], axis=1)

    held = {}
    if planned:
        held[two] = send(weight, two)
        early = take(weight, chunks[1:2])
        late = take(weight, chunks[:1] + chunks[2:])
        own = [late[0], early[0], *late[1:]]
        partner = flip(weight, core)
        held[two | core] = flip(held[two], core)
        for c, piece in enumerate(own):
            held[c, one] = send(piece, one)
            held[c, one | two] = send(held[c, one], two)
            for mask in (one, one | two):
                held[c, mask | core] = flip(held[c, mask], core)
        both = jnp.concatenate([packed, flip(packed, core)], axis=0)
        side = send(both, one)
        across = lax.ppermute(both, "pop", [(i, i ^ (one | two)) for i in range(0, pops, 2)])
        mine = jnp.concatenate([side, across], axis=0)
        theirs = flip(mine, core)
        rest = both.shape[0]
        everyone = jnp.concatenate([both, side, theirs[:rest], across + theirs[rest:]], axis=0)
    else:
        everyone = lax.all_gather(packed, "pop", axis=0, tiled=True)

    every_fitness = everyone[:, 0]
    every_seeds = everyone[:, 1:].reshape((overall,) + past_seeds.shape[1:])
    lower_count = jnp.sum((every_fitness[None, :] < every_fitness[:, None]).astype(jnp.float32), axis=1)
    equal_count = jnp.sum((every_fitness[None, :] == every_fitness[:, None]).astype(jnp.float32), axis=1)
    centered = (lower_count + 0.5 * (equal_count - 1.0)) / (overall - 1.0) - 0.5
    out_hits, in_hits = one_hots(every_seeds, width)
    scaled = (STEP_SCALE * centered)[:, None, None] * out_hits
    coupling = lax.dot_general(
        scaled.reshape(-1, width),
        in_hits.reshape(-1, width),
        (((0,), (0,)), ((), ())),
        precision=lax.Precision.HIGHEST,
    )

    span = bank_in.shape[0]
    banks = [bank_in]
    for step in range(1, lanes):
        banks.append(lax.ppermute(bank_in, "row", [(i, (i - step) % lanes) for i in range(lanes)]))
    if span % depth == 0:
        ring = (lane + jnp.arange(lanes, dtype=jnp.int32)) % lanes
        pick = jnp.concatenate([ring, jnp.stack([me * depth // span, me * depth % span])]).astype(jnp.int32)
        projected, columns = projections(pick, flat_tokens, banks, depth)
    else:
        full_in = jnp.zeros((features, width), bank_in.dtype)
        for step, block in enumerate(banks):
            full_in = lax.dynamic_update_slice_in_dim(full_in, block, ((lane + step) % lanes) * span, 0)
        projected = jnp.dot(flat_tokens, full_in, preferred_element_type=jnp.float32)
        columns = lax.dynamic_slice_in_dim(full_in, me * depth, depth, 0)
    low, right_part = lowrank(projected, coupling, new_seeds, columns)
    new_weight = updated(weight, bank_out, right_part)

    if planned:
        hidden, partial = None, []
        for c, (start, length) in enumerate(chunks):
            near = [(0, weight, start), (core, partner, start)] + [(m, held[c, m], 0) for m in (one, one | core)]
            part = product(flat_tokens, start, length, tile, rows, near, low=low, bank_out=bank_out)
            side = [(m, held[m], start) for m in (two, two | core)]
            partial.append(product(flat_tokens, start, length, tile, rows, side, partial=part))
        for c, (start, length) in enumerate(chunks):
            far = [(m, held[c, m], 0) for m in (6, 7)]
            if c > 1:
                partial[c] = product(flat_tokens, start, length, tile, rows, far[:1], partial=partial[c], resident=True)
                far = far[1:]
            hidden = product(flat_tokens, start, length, length if c > 1 and start % length == 0 else tile, rows, far, partial=partial[c], final=True, hidden=hidden, resident=c > 1)
    else:
        blocks = {0: weight}
        for bit in range((pops - 1).bit_length()):
            if pops & (pops - 1) == 0:
                blocks.update({m | 1 << bit: flip(b, 1 << bit) for m, b in list(blocks.items())})
        if len(blocks) == pops:
            full = jnp.zeros((rows, features), weight.dtype)
            for m, b in blocks.items():
                full = lax.dynamic_update_slice_in_dim(full, b, (me ^ m) * depth, 1)
        else:
            full = lax.all_gather(weight, "pop", axis=1, tiled=True)
        hidden = lax.dot_general(flat_tokens, full, DIMS, preferred_element_type=jnp.float32)
        hidden += lax.dot_general(low, jnp.concatenate([bank_out, bank_out], axis=1), DIMS, preferred_element_type=jnp.float32)
        hidden = hidden.astype(jnp.bfloat16)
    return (hidden.reshape(members, tokens.shape[1], rows), new_weight)


def solution(mesh):
    placed = (
        P("pop", None, None),
        P("row", "pop"),
        P("row", None),
        P("row", None),
        P("pop"),
        P("pop", None, None),
        P("pop", None, None),
    )
    return jax.shard_map(
        shards,
        mesh=mesh,
        in_specs=placed,
        out_specs=(P("pop", None, "row"), P("row", "pop")),
        check_vma=False,
    )
```
